32 devices in a mesh: dp: 4 (over y, z), ep: 8 (over x, core).
Axes of the slice: x: 4, y: 2, z: 2, core: 2. Of those that a mesh axis runs over, the one named last changes fastest.
The devices are a block of a 4x4x8 slice.
Arguments:
- hidden: bfloat16 [3072, 2048], P(('dp', 'ep')), parts along dimension 0
- norm_gain: bfloat16 [2048], replicated
- w_gate: bfloat16 [2048, 64], replicated
- w1_shared: bfloat16 [2048, 2816], replicated
- w3_shared: bfloat16 [2048, 2816], replicated
- w2_shared: bfloat16 [2816, 2048], replicated
- w1_experts: bfloat16 [64, 2048, 1408], P('ep')
- w3_experts: bfloat16 [64, 2048, 1408], P('ep')
- w2_experts: bfloat16 [64, 1408, 2048], P('ep')
- topk_ids: int32 [3072, 6], P(('dp', 'ep')), parts along dimension 0
Outputs:
- output: bfloat16 [3072, 2048], P(('dp', 'ep')), parts along dimension 0
There are 4 independent parts. The reference program is written for one: setup_inputs(seed, part) draws one part's arguments, and reference() takes and returns one part's arrays. A program takes and returns all parts, laid end to end along the dimension named above; an argument that names none is the same for every part.
All inputs are finite; a program needn't handle non-finite values.
Results may differ from the reference program's by a relative error of at most 0.00585255.
Values are sent between devices in bfloat16 or wider.
A program may use at most 768 MiB of HBM per device.

```python
import jax
import jax.numpy as jnp
from jax import lax

HIDDEN = 2048
EXPERTS = 64
EXPERT_FF = 1408
SHARED_FF = 2816
TOP_K = 6
TOKENS_DEV = 96
TOKENS = 768
GROUPS = 8
TOP_GROUPS = 3
ROUTE_SCALE = 16
NORM_EPS = 1e-6
GROUP_SIZE = EXPERTS // GROUPS


def draw_routing(route_key):
    blocks = TOKENS // TOKENS_DEV
    half_block = TOKENS_DEV // 2
    key_hot, key_cycle, key_perm, key_score, key_pick = jax.random.split(route_key, 5)
    hot_group = jax.random.randint(key_hot, (blocks, 1, 1), 0, GROUPS)
    cycle_off = jax.random.randint(key_cycle, (blocks, 1, 1), 0, GROUPS - 1)
    perm_keys = jax.random.split(key_perm, blocks)
    rank_in = jax.vmap(lambda sub_key: jax.random.permutation(sub_key, TOKENS_DEV))(perm_keys)[:, :, None]
    first_set = (rank_in * (TOP_GROUPS - 1) + jnp.arange(TOP_GROUPS - 1) + cycle_off) % (GROUPS - 1)
    first_groups = jnp.concatenate([jnp.broadcast_to(hot_group, (blocks, TOKENS_DEV, 1)), (hot_group + 1 + first_set) % GROUPS], axis=2)
    second_set = (rank_in * TOP_GROUPS + jnp.arange(TOP_GROUPS) + cycle_off) % (GROUPS - 1)
    second_groups = (hot_group + 1 + second_set) % GROUPS
    chosen = jnp.where(rank_in < half_block, first_groups, second_groups).reshape(TOKENS, TOP_GROUPS)
    scores = jax.random.randint(key_score, (TOKENS, TOP_GROUPS, GROUP_SIZE), 0, 2 ** 19) * 512
    scores = scores + jnp.arange(TOP_GROUPS * GROUP_SIZE).reshape(TOP_GROUPS, GROUP_SIZE)
    pick_idx = jax.random.randint(key_pick, (TOKENS, TOP_GROUPS, 1), 0, GROUP_SIZE)
    scores = scores + jnp.where(jnp.arange(GROUP_SIZE) == pick_idx, 2 ** 29, 0)
    cand_idx = lax.top_k(scores.reshape(TOKENS, TOP_GROUPS * GROUP_SIZE), TOP_K)[1]
    group_of = jnp.take_along_axis(chosen, cand_idx // GROUP_SIZE, axis=1)
    return (group_of * GROUP_SIZE + cand_idx % GROUP_SIZE).astype(jnp.int32)


def normal_bf16(sub_key, shape_in, scale_by):
    return (scale_by * jax.random.normal(sub_key, shape_in, jnp.float32)).astype(jnp.bfloat16)


def setup_inputs(seed: int = 0, part: int = 0) -> dict:
    part_key = jax.random.fold_in(jax.random.key(seed), part)
    weight_keys = jax.random.split(jax.random.key(seed + 1), 8)
    hidden = normal_bf16(jax.random.fold_in(part_key, 1), (TOKENS, HIDDEN), 0.5)
    norm_gain = (1.0 + 0.2 * jax.random.normal(weight_keys[0], (HIDDEN,), jnp.float32)).astype(jnp.bfloat16)
    w_gate = normal_bf16(weight_keys[1], (HIDDEN, EXPERTS), HIDDEN ** -0.5)
    w1_shared = normal_bf16(weight_keys[2], (HIDDEN, SHARED_FF), HIDDEN ** -0.5)
    w3_shared = normal_bf16(weight_keys[3], (HIDDEN, SHARED_FF), HIDDEN ** -0.5)
    w2_shared = normal_bf16(weight_keys[4], (SHARED_FF, HIDDEN), SHARED_FF ** -0.5)
    w1_experts = normal_bf16(weight_keys[5], (EXPERTS, HIDDEN, EXPERT_FF), HIDDEN ** -0.5)
    w3_experts = normal_bf16(weight_keys[6], (EXPERTS, HIDDEN, EXPERT_FF), HIDDEN ** -0.5)
    w2_experts = normal_bf16(weight_keys[7], (EXPERTS, EXPERT_FF, HIDDEN), EXPERT_FF ** -0.5)
    topk_ids = draw_routing(jax.random.fold_in(part_key, 2))
    return dict(hidden=hidden, norm_gain=norm_gain, w_gate=w_gate, w1_shared=w1_shared, w3_shared=w3_shared, w2_shared=w2_shared, w1_experts=w1_experts, w3_experts=w3_experts, w2_experts=w2_experts, topk_ids=topk_ids)


def rms_norm(hidden, norm_gain):
    rows_f = hidden.astype(jnp.float32)
    inv_rms = lax.rsqrt(jnp.mean(rows_f * rows_f, axis=-1, keepdims=True) + NORM_EPS)
    return (rows_f * inv_rms * norm_gain.astype(jnp.float32)).astype(jnp.bfloat16)


def swiglu(rows_in, w_up, w_lin, w_down):
    gate_act = jnp.dot(rows_in, w_up, preferred_element_type=jnp.float32)
    lin_act = jnp.dot(rows_in, w_lin, preferred_element_type=jnp.float32)
    inner_act = (jax.nn.silu(gate_act) * lin_act).astype(jnp.bfloat16)
    return jnp.dot(inner_act, w_down, preferred_element_type=jnp.float32).astype(jnp.bfloat16)


def reference(hidden, norm_gain, w_gate, w1_shared, w3_shared, w2_shared, w1_experts, w3_experts, w2_experts, topk_ids):
    normed = rms_norm(hidden, norm_gain)
    gate_probs = jax.nn.softmax(jnp.dot(normed, w_gate, preferred_element_type=jnp.float32), axis=-1)
    gate_wts = ROUTE_SCALE * jnp.take_along_axis(gate_probs, topk_ids, axis=1)
    shared_out = swiglu(normed, w1_shared, w3_shared, w2_shared)

    def expert_step(routed_acc, expert_in):
        w_up, w_lin, w_down, expert_id = expert_in
        column = jnp.sum(jnp.where(topk_ids == expert_id, gate_wts, 0.0), axis=1)
        expert_out = swiglu(normed, w_up, w_lin, w_down)
        return routed_acc + column[:, None] * expert_out.astype(jnp.float32), None

    routed = lax.scan(expert_step, jnp.zeros(hidden.shape, jnp.float32), (w1_experts, w3_experts, w2_experts, jnp.arange(EXPERTS)))[0]
    return (hidden.astype(jnp.float32) + shared_out.astype(jnp.float32) + routed).astype(jnp.bfloat16)
```

```python
import functools

import jax
import jax.numpy as jnp
from jax import lax
from jax.experimental import pallas as pl
from jax.experimental.pallas import tpu as pltpu
from jax.sharding import PartitionSpec as P

ROUTE_SCALE = 16
NORM_EPS = 1e-6
CAP = 128
K_CHUNKS = 4
J_CHUNKS = 8
UP_SLOTS = 5
DOWN_SLOTS = 8
LAG = 2

F32 = jnp.float32
BF16 = jnp.bfloat16


def rms_norm(hidden, norm_gain):
    rows_f = hidden.astype(F32)
    inv_rms = lax.rsqrt(jnp.mean(rows_f * rows_f, axis=-1, keepdims=True) + NORM_EPS)
    return (rows_f * inv_rms * norm_gain.astype(F32)).astype(BF16)


def swiglu(rows_in, w_up, w_lin, w_down):
    gate_act = jnp.dot(rows_in, w_up, preferred_element_type=F32)
    lin_act = jnp.dot(rows_in, w_lin, preferred_element_type=F32)
    inner_act = (jax.nn.silu(gate_act) * lin_act).astype(BF16)
    return jnp.dot(inner_act, w_down, preferred_element_type=F32).astype(BF16)


def dense_path(n, hidden, norm_gain, w_gate, w1_shared, w3_shared, w2_shared, w1_experts, w3_experts, w2_experts, topk_ids):
    normed = rms_norm(hidden, norm_gain)
    probs = jax.nn.softmax(jnp.dot(normed, w_gate, preferred_element_type=F32), axis=-1)
    gate_wts = ROUTE_SCALE * jnp.take_along_axis(probs, topk_ids, axis=1)
    shared_out = swiglu(normed, w1_shared, w3_shared, w2_shared)
    pieces = 4
    width = normed.shape[1] // pieces
    gathered = [
        lax.all_gather(normed[:, i * width : (i + 1) * width], 'ep', axis=0, tiled=True) for i in range(pieces)
    ]
    all_rows = jnp.concatenate(gathered, axis=1)
    all_ids = lax.all_gather(topk_ids, 'ep', axis=0, tiled=True)
    all_wts = lax.all_gather(gate_wts, 'ep', axis=0, tiled=True)
    local_count = w1_experts.shape[0]
    first = lax.axis_index('ep') * local_count

    def one_expert(acc, xs):
        w_up, w_lin, w_down, expert = xs
        column = jnp.sum(jnp.where(all_ids == expert, all_wts, 0.0), axis=1)
        return acc + column[:, None] * swiglu(all_rows, w_up, w_lin, w_down).astype(F32), None

    part, _ = lax.scan(
        one_expert, jnp.zeros(all_rows.shape, F32), (w1_experts, w3_experts, w2_experts, first + jnp.arange(local_count))
    )
    back = lax.all_to_all(part.reshape(n, hidden.shape[0], -1), 'ep', split_axis=0, concat_axis=0)
    return (hidden.astype(F32) + shared_out.astype(F32) + jnp.sum(back, axis=0)).astype(BF16)


def moe_kernel(
    n, hid_hbm, gain_hbm, wg_hbm, w1s, w3s, w2s, w1e, w3e, w2e, ids_hbm,
    out_ref, most_ref,
    hid, gain, wg, ids, tile, info, wmap, rank, x_all, xg, gsel, ssel, wb, acc1, acc3, inner, ebuf,
    sacc1, sacc3, sinner, sh, part, from_sib, from_tr, from_fin, abuf, bbuf,
    in_sem, info_send, info_recv, ag_send, ag_recv, a_sem, b_sem,
    sib_send, sib_recv, tr_send, tr_recv, dir_send, com_send, fin_recv,
):
    rows, width = hid.shape
    experts, _, ff = w1e.shape
    total = n * rows
    chips = n // 2
    kd = width // K_CHUNKS
    jd = width // J_CHUNKS
    halves = w1s.shape[1] // ff
    n_shared = K_CHUNKS * halves
    n_up = K_CHUNKS * experts
    n_down = J_CHUNKS * experts
    n_down_all = n_down + J_CHUNKS * halves

    me = lax.axis_index('ep')
    chip, core = me // 2, lax.rem(me, 2)

    def dev(c, k):
        return lax.rem(c + chips, chips) * 2 + k

    right, left, sib = dev(chip + 1, core), dev(chip - 1, core), dev(chip, 1 - core)
    far = dev(chip + 2, core)

    def block(b):
        return pl.ds(pl.multiple_of(b * rows, 16), rows)

    small = [
        pltpu.make_async_copy(src, dst, in_sem.at[i])
        for i, (src, dst) in enumerate(((hid_hbm, hid), (gain_hbm, gain), (wg_hbm, wg), (ids_hbm, ids)))
    ]
    for copy in small:
        copy.start()

    def up_pair(pair, slot):
        return [pltpu.make_async_copy(src, abuf.at[slot, i], a_sem.at[slot, i]) for i, src in enumerate(pair)]

    def up_shared(s):
        k, h = s // halves, lax.rem(s, halves)
        at = (pl.ds(pl.multiple_of(k * kd, 128), kd), pl.ds(pl.multiple_of(h * ff, 128), ff))
        return up_pair((w1s.at[at], w3s.at[at]), lax.rem(s, UP_SLOTS))

    def up_routed(q):
        k, e = q // experts, lax.rem(q, experts)
        at = (e, pl.ds(pl.multiple_of(k * kd, 128), kd))
        return up_pair((w1e.at[at], w3e.at[at]), lax.rem(q + n_shared, UP_SLOTS))

    def down_routed(q):
        j, e = q // experts, lax.rem(q, experts)
        src = w2e.at[e, :, pl.ds(pl.multiple_of(j * jd, 128), jd)]
        slot = lax.rem(q, DOWN_SLOTS)
        return pltpu.make_async_copy(src, bbuf.at[slot], b_sem.at[slot])

    def down_shared(q):
        j, h = q // halves, lax.rem(q, halves)
        src = w2s.at[pl.ds(pl.multiple_of(h * ff, 128), ff), pl.ds(pl.multiple_of(j * jd, 128), jd)]
        slot = lax.rem(q + n_down, DOWN_SLOTS)
        return pltpu.make_async_copy(src, bbuf.at[slot], b_sem.at[slot])

    def start_up(s):
        if isinstance(s, int):
            if s < n_shared:
                for copy in up_shared(jnp.int32(s)):
                    copy.start()
            elif s < n_shared + n_up:
                for copy in up_routed(jnp.int32(s - n_shared)):
                    copy.start()
            return

        @pl.when(s < n_shared)
        def _():
            for copy in up_shared(s):
                copy.start()

        @pl.when((s >= n_shared) & (s < n_shared + n_up))
        def _():
            for copy in up_routed(s - n_shared):
                copy.start()

    def start_down(q):
        @pl.when(q < n_down)
        def _():
            down_routed(q).start()

        @pl.when((q >= n_down) & (q < n_down_all))
        def _():
            down_shared(q - n_down).start()

    for s in range(UP_SLOTS):
        start_up(s)
    for q in range(DOWN_SLOTS):
        down_routed(jnp.int32(q)).start()

    barrier = pltpu.get_barrier_semaphore()
    for i in range(1, n):
        pl.semaphore_signal(
            barrier, inc=1, device_id={'ep': lax.rem(me + i, n)}, device_id_type=pl.DeviceIdType.MESH
        )

    for copy in small:
        copy.wait()
    rows_f = hid[...].astype(F32)
    inv_rms = lax.rsqrt(jnp.mean(rows_f * rows_f, axis=-1, keepdims=True) + NORM_EPS)
    for k in range(K_CHUNKS):
        cols = slice(k * kd, (k + 1) * kd)
        x_all[k, block(me), :] = (rows_f[:, cols] * inv_rms * gain[:, cols].astype(F32)).astype(BF16)
    pl.semaphore_wait(barrier, n - 1)

    def remote(src, dst, send, recv, to):
        return pltpu.make_async_remote_copy(
            src_ref=src, dst_ref=dst, send_sem=send, recv_sem=recv, device_id={'ep': to}, device_id_type=pl.DeviceIdType.MESH
        )

    def rows_copy(k, b, lane, to):
        at = (k, block(b))
        return remote(x_all.at[at], x_all.at[at], ag_send.at[k, lane], ag_recv.at[k, b], to)

    def send_own(k):
        rows_copy(k, me, 0, right).start()
        rows_copy(k, me, 1, left).start()
        rows_copy(k, me, 2, sib).start()

    def forward_near(k):
        rows_copy(k, left, 3, sib).wait_recv()
        rows_copy(k, right, 4, sib).wait_recv()
        even = lax.rem(k, 2) == 0
        onward = jnp.where(even, left, right)
        to = jnp.where(even, right, left)
        rows_copy(k, onward, 5, to).start()
        rows_copy(k, left, 3, sib).start()
        rows_copy(k, right, 4, sib).start()

    def forward_far(k):
        rows_copy(k, far, 6, sib).wait_recv()
        rows_copy(k, far, 6, sib).start()

    def wait_sib_rows(k):
        for i in range(chips):
            rows_copy(k, dev(chip + i, 1 - core), 0, sib).wait_recv()

    send_own(0)
    send_own(1)

    logits = jnp.concatenate([x_all[k, block(me), :] for k in range(K_CHUNKS)], axis=1)
    logits = jnp.dot(logits, wg[...], preferred_element_type=F32)
    expd = jnp.exp(logits - jnp.max(logits, axis=-1, keepdims=True))
    probs = expd / jnp.sum(expd, axis=-1, keepdims=True)
    top_k = ids.shape[1]
    expert_lane = lax.broadcasted_iota(jnp.int32, probs.shape, 1)
    lane = lax.broadcasted_iota(jnp.int32, (rows, 128), 1)
    packed = jnp.zeros((rows, 128), F32)
    for i in range(top_k):
        col = ids[:, i : i + 1]
        wt = ROUTE_SCALE * jnp.sum(jnp.where(expert_lane == col, probs, 0.0), axis=-1, keepdims=True)
        packed = jnp.where(lane == i, wt, packed)
        packed = jnp.where(lane == 8 + i, col.astype(F32), packed)
    tile[...] = jnp.zeros_like(tile)
    tile[0:rows, :] = packed
    info[me] = tile[...].T[0:16, :]

    def info_copy(i, b, to):
        return remote(info.at[b], info.at[b], info_send.at[i], info_recv.at[b], to)

    def shared_step(s, _):
        k, h = s // halves, lax.rem(s, halves)
        for copy in up_shared(s):
            copy.wait()
        slot = lax.rem(s, UP_SLOTS)
        x = x_all[k, block(me), :]
        for i, acc in enumerate((sacc1, sacc3)):
            d = jnp.dot(x, abuf[slot, i], preferred_element_type=F32)

            @pl.when(k == 0)
            def _():
                acc[h] = d

            @pl.when(k > 0)
            def _():
                acc[h] = acc[h] + d

        start_up(s + UP_SLOTS)

        @pl.when(s == 0)
        def _():
            for i in range(1, n):
                info_copy(i, me, lax.rem(me + i, n)).start()

        @pl.when(s == 3)
        def _():
            forward_near(jnp.int32(0))
            send_own(jnp.int32(2))

        @pl.when(s == 6)
        def _():
            forward_near(jnp.int32(1))
            send_own(jnp.int32(3))

        return 0

    lax.fori_loop(0, n_shared, shared_step, 0)

    for i in range(1, n):
        b = lax.rem(me + i, n)
        info_copy(i, b, b).wait_recv()
    info_cols = info[...].reshape(n * 16, 128).T
    first = (me * experts).astype(F32)
    all_experts = float(n * experts)
    lane_f = lax.broadcasted_iota(jnp.int32, (rows, 128), 1).astype(F32)
    lower = lax.broadcasted_iota(jnp.int32, (rows, rows), 0) > lax.broadcasted_iota(jnp.int32, (rows, rows), 1)
    lower = jnp.where(lower, 1.0, 0.0).astype(BF16)
    seen = jnp.zeros((1, 128), F32)
    for b in range(n):
        wm = jnp.zeros((rows, 128), F32)
        hit_any = jnp.zeros((rows, 128), F32)
        for i in range(top_k):
            wt = info_cols[0:rows, 16 * b + i : 16 * b + i + 1]
            at = info_cols[0:rows, 16 * b + 8 + i : 16 * b + 9 + i] - first
            at = jnp.where(at < 0, at + all_experts, at)
            hit = lane_f == at
            wm = jnp.where(hit, wt, wm)
            hit_any = jnp.where(hit, 1.0, hit_any)
        before = jnp.dot(lower, hit_any.astype(BF16), preferred_element_type=F32) + seen
        wmap[b * rows : (b + 1) * rows, :] = wm
        rank[b * rows : (b + 1) * rows, :] = jnp.where(hit_any > 0, before, -1.0)
        seen = seen + jnp.sum(hit_any, axis=0, keepdims=True)
    most_ref[...] = jnp.broadcast_to(jnp.max(seen, axis=1, keepdims=True), most_ref.shape)
    rank_rows = rank[...].T
    place = lax.broadcasted_iota(jnp.int32, (CAP, total), 0).astype(F32)
    for e in range(experts):
        hit = place == jnp.broadcast_to(rank_rows[e : e + 1, :], (CAP, total))
        gsel[e * CAP : (e + 1) * CAP, :] = jnp.where(hit, 1.0, 0.0).astype(BF16)

    forward_far(jnp.int32(0))

    def up_chunk(k, _):
        wait_sib_rows(k)
        for half in range(2):
            span = slice(half * experts * CAP // 2, (half + 1) * experts * CAP // 2)
            xg[span, :] = jnp.dot(gsel[span, :], x_all[k], preferred_element_type=F32).astype(BF16)

        def up_step(e, _):
            q = k * experts + e
            for copy in up_routed(q):
                copy.wait()
            slot = lax.rem(q + n_shared, UP_SLOTS)
            x = xg[pl.ds(pl.multiple_of(e * CAP, CAP), CAP), :]
            for i, acc in enumerate((acc1, acc3)):
                d = jnp.dot(x, abuf[slot, i], preferred_element_type=F32)

                @pl.when(k == 0)
                def _():
                    acc[e] = d

                @pl.when(k > 0)
                def _():
                    acc[e] = acc[e] + d

            start_up(q + n_shared + UP_SLOTS)

            @pl.when((e == 3) & (k + 1 < K_CHUNKS))
            def _():
                forward_far(k + 1)

            @pl.when((e == 3) & (k + 2 < K_CHUNKS))
            def _():
                forward_near(k + 2)

            return 0

        lax.fori_loop(0, experts, up_step, 0)

        @pl.when(k == 1)
        def _():
            slots = lax.broadcasted_iota(jnp.int32, (total, CAP), 1).astype(F32)
            ranks = rank[...]
            wts = wmap[...]
            for e in range(experts):
                hit = slots == jnp.broadcast_to(ranks[:, e : e + 1], (total, CAP))
                ssel[e] = jnp.where(hit, 1.0, 0.0).astype(BF16)
                wb[e] = jnp.broadcast_to(wts[:, e : e + 1], (total, 128))

        return 0

    lax.fori_loop(0, K_CHUNKS, up_chunk, 0)

    def activate(e, _):
        inner[e] = (jax.nn.silu(acc1[e]) * acc3[e]).astype(BF16)
        return 0

    lax.fori_loop(0, experts, activate, 0)
    for h in range(halves):
        sinner[h] = (jax.nn.silu(sacc1[h]) * sacc3[h]).astype(BF16)

    def sib_copy(j, c):
        return remote(
            part.at[j, block(c * 2 + (1 - core))], from_sib.at[j, c], sib_send.at[j, c], sib_recv.at[j, c], sib
        )

    def step_of(j):
        return 1 - 2 * lax.rem(j, 2)

    def tr_copy(j):
        d = step_of(j)
        return remote(part.at[j, block(far)], from_tr.at[j], tr_send.at[j], tr_recv.at[j], dev(chip + d, core))

    def dir_copy(j):
        to = dev(chip - step_of(j), core)
        return remote(part.at[j, block(to)], from_fin.at[1, j], dir_send.at[j], fin_recv.at[1, j], to)

    def com_copy(j):
        to = dev(chip + step_of(j), core)
        return remote(part.at[j, block(to)], from_fin.at[0, j], com_send.at[j], fin_recv.at[0, j], to)

    def down_range(j, _):
        @pl.when(j < J_CHUNKS)
        def _():
            def down_step(g, _):
                for u in range(4):
                    e = g * 4 + u
                    q = j * experts + e
                    down_routed(q).wait()
                    d = jnp.dot(inner[e], bbuf[lax.rem(q, DOWN_SLOTS)], preferred_element_type=F32)
                    ebuf[e] = d.astype(BF16)
                for u in range(4):
                    start_down(j * experts + g * 4 + u + DOWN_SLOTS)
                return 0

            lax.fori_loop(0, experts // 4, down_step, 0)

            def spread(m, _):
                span = pl.ds(pl.multiple_of(m * 128, 128), 128)
                acc = jnp.zeros((128, jd), F32)
                for e in range(experts):
                    d = jnp.dot(ssel[e, span, :], ebuf[e], preferred_element_type=F32)
                    wt = wb[e, span, :]
                    if jd > 128:
                        wt = jnp.concatenate([wt] * (jd // 128), axis=1)
                    elif jd < 128:
                        wt = wt[:, :jd]
                    acc = acc + d * wt
                part[j, span, :] = acc
                return 0

            lax.fori_loop(0, total // 128, spread, 0)

        @pl.when((j >= 1) & (j <= J_CHUNKS))
        def _():
            for c in range(chips):
                sib_copy(j - 1, c).wait_recv()
                at = (j - 1, block(c * 2 + core))
                part[at] = part[at] + from_sib[j - 1, c]

        @pl.when(j >= LAG)
        def _():
            i = j - LAG
            tr_copy(i).wait_recv()
            at = (i, block(dev(chip + step_of(i), core)))
            part[at] = part[at] + from_tr[i]

        @pl.when((j >= 1) & (j <= J_CHUNKS))
        def _():
            dir_copy(j - 1).start()
            tr_copy(j - 1).start()

        @pl.when(j >= LAG)
        def _():
            com_copy(j - LAG).start()

        @pl.when(j < J_CHUNKS)
        def _():
            for c in range(chips):
                sib_copy(j, c).start()

        return 0

    lax.fori_loop(0, J_CHUNKS + LAG, down_range, 0)

    def shared_down(j, _):
        acc = jnp.zeros((rows, jd), F32)
        for h in range(halves):
            q = j * halves + h
            down_shared(q).wait()
            acc = acc + jnp.dot(sinner[h], bbuf[lax.rem(q + n_down, DOWN_SLOTS)], preferred_element_type=F32)
        sh[j] = acc
        for h in range(halves):
            start_down(n_down + j * halves + h + DOWN_SLOTS)
        return 0

    lax.fori_loop(0, J_CHUNKS, shared_down, 0)

    for j in range(J_CHUNKS):
        cols = slice(j * jd, (j + 1) * jd)
        com_copy(jnp.int32(j)).wait_recv()
        dir_copy(jnp.int32(j)).wait_recv()
        routed = part[j, block(me), :] + (from_fin[0, j] + from_fin[1, j])
        shared_out = sh[j].astype(BF16).astype(F32)
        out_ref[:, cols] = (hid[:, cols].astype(F32) + shared_out + routed).astype(BF16)

    for i in range(1, n):
        info_copy(i, me, lax.rem(me + i, n)).wait_send()
    for k in range(K_CHUNKS):
        for lane_i in range(7):
            rows_copy(jnp.int32(k), me, lane_i, sib).wait_send()
    for j in range(J_CHUNKS):
        ji = jnp.int32(j)
        for c in range(chips):
            sib_copy(ji, c).wait_send()
        tr_copy(ji).wait_send()
        dir_copy(ji).wait_send()
        com_copy(ji).wait_send()


def routed_layer(n, *args):
    hidden, norm_gain, w_gate, w1_shared, w3_shared, w2_shared, w1_experts, w3_experts, w2_experts, topk_ids = args
    rows, width = hidden.shape
    experts, _, ff = w1_experts.shape
    total = n * rows
    chips = n // 2
    kd = width // K_CHUNKS
    jd = width // J_CHUNKS
    halves = w1_shared.shape[1] // ff
    dma = pltpu.SemaphoreType.DMA
    vmem = pltpu.VMEM
    scratch = [
        vmem((rows, width), BF16),
        vmem((1, width), BF16),
        vmem(w_gate.shape, BF16),
        vmem(topk_ids.shape, jnp.int32),
        vmem((128, 128), F32),
        vmem((n, 16, 128), F32),
        vmem((total, 128), F32),
        vmem((total, 128), F32),
        vmem((K_CHUNKS, total, kd), BF16),
        vmem((experts * CAP, kd), BF16),
        vmem((experts * CAP, total), BF16),
        vmem((experts, total, CAP), BF16),
        vmem((experts, total, 128), F32),
        vmem((experts, CAP, ff), F32),
        vmem((experts, CAP, ff), F32),
        vmem((experts, CAP, ff), BF16),
        vmem((experts, CAP, jd), BF16),
        vmem((halves, rows, ff), F32),
        vmem((halves, rows, ff), F32),
        vmem((halves, rows, ff), BF16),
        vmem((J_CHUNKS, rows, jd), F32),
        vmem((J_CHUNKS, total, jd), F32),
        vmem((J_CHUNKS, chips, rows, jd), F32),
        vmem((J_CHUNKS, rows, jd), F32),
        vmem((2, J_CHUNKS, rows, jd), F32),
        vmem((UP_SLOTS, 2, kd, ff), BF16),
        vmem((DOWN_SLOTS, ff, jd), BF16),
        dma((4,)),
        dma((n,)),
        dma((n,)),
        dma((K_CHUNKS, 7)),
        dma((K_CHUNKS, n)),
        dma((UP_SLOTS, 2)),
        dma((DOWN_SLOTS,)),
        dma((J_CHUNKS, chips)),
        dma((J_CHUNKS, chips)),
        dma((J_CHUNKS,)),
        dma((J_CHUNKS,)),
        dma((J_CHUNKS,)),
        dma((J_CHUNKS,)),
        dma((2, J_CHUNKS)),
    ]
    return pl.pallas_call(
        functools.partial(moe_kernel, n),
        out_shape=[jax.ShapeDtypeStruct((rows, width), BF16), jax.ShapeDtypeStruct((8, 128), F32)],
        in_specs=[pl.BlockSpec(memory_space=pl.ANY)] * 10,
        out_specs=[pl.BlockSpec(memory_space=pltpu.VMEM)] * 2,
        scratch_shapes=scratch,
        compiler_params=pltpu.CompilerParams(collective_id=0, has_side_effects=True, vmem_limit_bytes=67043328),
        name='moe_layer',
    )(hidden, norm_gain.reshape(1, width), *args[2:])


def solution(mesh):
    n = mesh.shape['ep']
    tok_spec = P(('dp', 'ep'), None)
    expert_spec = P('ep', None, None)

    def local_fn(*args):
        out, most = routed_layer(n, *args)
        return lax.cond(most[0, 0] > CAP, lambda: dense_path(n, *args), lambda: out)

    return jax.shard_map(local_fn, mesh=mesh, in_specs=(tok_spec, P(), P(), P(), P(), P(), expert_spec, expert_spec, expert_spec, tok_spec), out_specs=tok_spec, check_vma=False)
```

```python
import functools

import jax
import jax.numpy as jnp
from jax import lax
from jax.experimental import pallas as pl
from jax.experimental.pallas import tpu as pltpu
from jax.sharding import PartitionSpec as P

ROUTE_SCALE = 16
NORM_EPS = 1e-6
CAP = 128
K_CHUNKS = 4
J_CHUNKS = 8
N_CHUNKS = 4
UP_SLOTS = 7

F32 = jnp.float32
BF16 = jnp.bfloat16


def rms_norm(hidden, norm_gain):
    rows_f = hidden.astype(F32)
    inv_rms = lax.rsqrt(jnp.mean(rows_f * rows_f, axis=-1, keepdims=True) + NORM_EPS)
    return (rows_f * inv_rms * norm_gain.astype(F32)).astype(BF16)


def swiglu(rows_in, w_up, w_lin, w_down):
    gate_act = jnp.dot(rows_in, w_up, preferred_element_type=F32)
    lin_act = jnp.dot(rows_in, w_lin, preferred_element_type=F32)
    inner_act = (jax.nn.silu(gate_act) * lin_act).astype(BF16)
    return jnp.dot(inner_act, w_down, preferred_element_type=F32).astype(BF16)


def dense_path(n, hidden, norm_gain, w_gate, w1_shared, w3_shared, w2_shared, w1_experts, w3_experts, w2_experts, topk_ids):
    normed = rms_norm(hidden, norm_gain)
    probs = jax.nn.softmax(jnp.dot(normed, w_gate, preferred_element_type=F32), axis=-1)
    gate_wts = ROUTE_SCALE * jnp.take_along_axis(probs, topk_ids, axis=1)
    shared_out = swiglu(normed, w1_shared, w3_shared, w2_shared)
    pieces = 4
    width = normed.shape[1] // pieces
    gathered = [
        lax.all_gather(normed[:, i * width : (i + 1) * width], 'ep', axis=0, tiled=True) for i in range(pieces)
    ]
    all_rows = jnp.concatenate(gathered, axis=1)
    all_ids = lax.all_gather(topk_ids, 'ep', axis=0, tiled=True)
    all_wts = lax.all_gather(gate_wts, 'ep', axis=0, tiled=True)
    local_count = w1_experts.shape[0]
    first = lax.axis_index('ep') * local_count

    def one_expert(acc, xs):
        w_up, w_lin, w_down, expert = xs
        column = jnp.sum(jnp.where(all_ids == expert, all_wts, 0.0), axis=1)
        return acc + column[:, None] * swiglu(all_rows, w_up, w_lin, w_down).astype(F32), None

    part, _ = lax.scan(
        one_expert, jnp.zeros(all_rows.shape, F32), (w1_experts, w3_experts, w2_experts, first + jnp.arange(local_count))
    )
    back = lax.all_to_all(part.reshape(n, hidden.shape[0], -1), 'ep', split_axis=0, concat_axis=0)
    return (hidden.astype(F32) + shared_out.astype(F32) + jnp.sum(back, axis=0)).astype(BF16)


def moe_kernel(
    n, hid_hbm, gain_hbm, wg_hbm, w1s, w3s, w2s, w1e, w3e, w2e, ids_hbm,
    out_ref, over_ref,
    hid, gain, wg, ids, tile, info, wmap, rank, x_all, ssel, wb, inner, sinner, sh,
    from_sib, from_tr, from_fin, bbuf,
    in_sem, info_send, info_recv, ag_send, ag_recv, a_sem, b_sem,
    sib_send, sib_recv, tr_send, tr_recv, dir_send, com_send, fin_recv,
):
    rows, width = hid.shape
    experts, _, ff = w1e.shape
    total = n * rows
    chips = n // 2
    kd = width // K_CHUNKS
    jd = width // J_CHUNKS
    nd = width // N_CHUNKS
    per = nd // jd
    halves = w1s.shape[1] // ff
    n_shared = K_CHUNKS * halves
    n_up = K_CHUNKS * experts
    slots = experts // 2

    me = lax.axis_index('ep')
    chip, core = me // 2, lax.rem(me, 2)

    def dev(c, k):
        return lax.rem(c + chips, chips) * 2 + k

    right, left, sib = dev(chip + 1, core), dev(chip - 1, core), dev(chip, 1 - core)
    far = dev(chip + 2, core)

    def block(b):
        return pl.ds(pl.multiple_of(b * rows, 16), rows)

    small = [
        pltpu.make_async_copy(src, dst, in_sem.at[i])
        for i, (src, dst) in enumerate(((hid_hbm, hid), (gain_hbm, gain), (wg_hbm, wg), (ids_hbm, ids)))
    ]
    for copy in small:
        copy.start()

    def down_routed(t, e, buf, slot, sem):
        src = w2e.at[e, :, pl.ds(pl.multiple_of(t * nd, 128), nd)]
        return pltpu.make_async_copy(src, buf.at[slot], b_sem.at[sem])

    def down_shared(q, buf, slot, sem):
        t, h = q // halves, lax.rem(q, halves)
        src = w2s.at[pl.ds(pl.multiple_of(h * ff, 128), ff), pl.ds(pl.multiple_of(t * nd, 128), nd)]
        return pltpu.make_async_copy(src, buf.at[slot], b_sem.at[sem])

    barrier = pltpu.get_barrier_semaphore()
    for i in range(1, n):
        pl.semaphore_signal(
            barrier, inc=1, device_id={'ep': lax.rem(me + i, n)}, device_id_type=pl.DeviceIdType.MESH
        )

    def remote(src, dst, send, recv, to):
        return pltpu.make_async_remote_copy(
            src_ref=src, dst_ref=dst, send_sem=send, recv_sem=recv, device_id={'ep': to}, device_id_type=pl.DeviceIdType.MESH
        )

    def phase_one(xg, gsel, acc1, acc3, sacc1, sacc3, abuf):
        def up_pair(pair, slot):
            return [pltpu.make_async_copy(src, abuf.at[slot, i], a_sem.at[slot, i]) for i, src in enumerate(pair)]

        def up_shared(s):
            k, h = s // halves, lax.rem(s, halves)
            at = (pl.ds(pl.multiple_of(k * kd, 128), kd), pl.ds(pl.multiple_of(h * ff, 128), ff))
            return up_pair((w1s.at[at], w3s.at[at]), lax.rem(s, UP_SLOTS))

        def up_routed(q):
            k, e = q // experts, lax.rem(q, experts)
            at = (e, pl.ds(pl.multiple_of(k * kd, 128), kd))
            return up_pair((w1e.at[at], w3e.at[at]), lax.rem(q + n_shared, UP_SLOTS))

        def start_up(s):
            if isinstance(s, int):
                if s < n_shared:
                    for copy in up_shared(jnp.int32(s)):
                        copy.start()
                elif s < n_shared + n_up:
                    for copy in up_routed(jnp.int32(s - n_shared)):
                        copy.start()
                return

            @pl.when(s < n_shared)
            def _():
                for copy in up_shared(s):
                    copy.start()

            @pl.when((s >= n_shared) & (s < n_shared + n_up))
            def _():
                for copy in up_routed(s - n_shared):
                    copy.start()

        with jax.named_scope('small_in'):
            for copy in small:
                copy.wait()
        for s in range(UP_SLOTS):
            start_up(s)
        for e in range(experts // 2):
            down_routed(0, e, bbuf, e, e).start()
        with jax.named_scope('norm'):
            rows_f = hid[...].astype(F32)
            inv_rms = lax.rsqrt(jnp.mean(rows_f * rows_f, axis=-1, keepdims=True) + NORM_EPS)
            for k in range(K_CHUNKS):
                cols = slice(k * kd, (k + 1) * kd)
                x_all[k, block(me), :] = (rows_f[:, cols] * inv_rms * gain[:, cols].astype(F32)).astype(BF16)
        with jax.named_scope('barrier'):
            pl.semaphore_wait(barrier, n - 1)

        def rows_copy(k, b, lane, to):
            at = (k, block(b))
            return remote(x_all.at[at], x_all.at[at], ag_send.at[k, lane], ag_recv.at[k, b], to)

        def send_own(k):
            rows_copy(k, me, 0, right).start()
            rows_copy(k, me, 1, left).start()
            rows_copy(k, me, 2, sib).start()

        def forward_near(k):
            rows_copy(k, left, 3, sib).wait_recv()
            rows_copy(k, right, 4, sib).wait_recv()
            even = lax.rem(k, 2) == 0
            onward = jnp.where(even, left, right)
            to = jnp.where(even, right, left)
            rows_copy(k, onward, 5, to).start()
            rows_copy(k, left, 3, sib).start()
            rows_copy(k, right, 4, sib).start()

        def forward_far(k):
            rows_copy(k, far, 6, sib).wait_recv()
            rows_copy(k, far, 6, sib).start()

        def wait_sib_rows(k):
            for i in range(chips):
                rows_copy(k, dev(chip + i, 1 - core), 0, sib).wait_recv()

        send_own(0)
        send_own(1)

        logits = jnp.concatenate([x_all[k, block(me), :] for k in range(K_CHUNKS)], axis=1)
        logits = lax.dot_general(logits, wg[...], (((1,), (1,)), ((), ())), preferred_element_type=F32)
        expd = jnp.exp(logits - jnp.max(logits, axis=-1, keepdims=True))
        probs = expd / jnp.sum(expd, axis=-1, keepdims=True)
        top_k = ids.shape[0]
        tile[...] = jnp.zeros_like(tile)
        tile[0:top_k, 0:rows] = ids[...].astype(F32)
        id_cols = tile[...].T[0:rows, :]
        expert_lane = lax.broadcasted_iota(jnp.int32, probs.shape, 1).astype(F32)
        lane = lax.broadcasted_iota(jnp.int32, (rows, 128), 1)
        packed = jnp.zeros((rows, 128), F32)
        for i in range(top_k):
            col = id_cols[:, i : i + 1]
            wt = ROUTE_SCALE * jnp.sum(jnp.where(expert_lane == col, probs, 0.0), axis=-1, keepdims=True)
            packed = jnp.where(lane == i, wt, packed)
            packed = jnp.where(lane == 8 + i, col, packed)
        tile[...] = jnp.zeros_like(tile)
        tile[0:rows, :] = packed
        info[me] = tile[...].T[0:16, :]

        def info_copy(i, b, to):
            return remote(info.at[b], info.at[b], info_send.at[i], info_recv.at[b], to)

        def shared_step(s, _):
            k, h = s // halves, lax.rem(s, halves)
            for copy in up_shared(s):
                copy.wait()
            slot = lax.rem(s, UP_SLOTS)
            x = x_all[k, block(me), :]
            for i, acc in enumerate((sacc1, sacc3)):
                d = jnp.dot(x, abuf[slot, i], preferred_element_type=F32)
                acc[h] = d + jnp.where(k == 0, 0.0, acc[h])

            start_up(s + UP_SLOTS)

            @pl.when(s == 0)
            def _():
                for i in range(1, n):
                    info_copy(i, me, lax.rem(me + i, n)).start()

            @pl.when(s == 3)
            def _():
                forward_near(jnp.int32(0))
                send_own(jnp.int32(2))

            @pl.when(s == 6)
            def _():
                forward_near(jnp.int32(1))
                send_own(jnp.int32(3))

            return 0

        with jax.named_scope('shared_up'):
            lax.fori_loop(0, n_shared, shared_step, 0)

        for i in range(1, n):
            b = lax.rem(me + i, n)
            info_copy(i, b, b).wait_recv()
        info_cols = info[...].reshape(n * 16, 128).T
        first = (me * experts).astype(F32)
        all_experts = float(n * experts)
        lane_f = lax.broadcasted_iota(jnp.int32, (rows, 128), 1).astype(F32)
        lower = lax.broadcasted_iota(jnp.int32, (rows, rows), 0) > lax.broadcasted_iota(jnp.int32, (rows, rows), 1)
        lower = jnp.where(lower, 1.0, 0.0).astype(BF16)
        seen = jnp.zeros((1, 128), F32)
        for b in range(n):
            wm = jnp.zeros((rows, 128), F32)
            hit_any = jnp.zeros((rows, 128), F32)
            for i in range(top_k):
                wt = info_cols[0:rows, 16 * b + i : 16 * b + i + 1]
                at = info_cols[0:rows, 16 * b + 8 + i : 16 * b + 9 + i] - first
                at = jnp.where(at < 0, at + all_experts, at)
                hit = lane_f == at
                wm = jnp.where(hit, wt, wm)
                hit_any = jnp.where(hit, 1.0, hit_any)
            before = jnp.dot(lower, hit_any.astype(BF16), preferred_element_type=F32) + seen
            wmap[b * rows : (b + 1) * rows, :] = wm
            rank[b * rows : (b + 1) * rows, :] = jnp.where(hit_any > 0, before, -1.0)
            seen = seen + jnp.sum(hit_any, axis=0, keepdims=True)
        over_ref[0, 0] = (jnp.max(seen) > CAP).astype(jnp.int32)
        rank_rows = rank[...].T
        place = lax.broadcasted_iota(jnp.int32, (CAP, total), 0).astype(F32)
        for e in range(experts):
            hit = place == jnp.broadcast_to(rank_rows[e : e + 1, :], (CAP, total))
            gsel[e * CAP : (e + 1) * CAP, :] = jnp.where(hit, 1.0, 0.0).astype(BF16)

        forward_far(jnp.int32(0))

        def up_chunk(k, _):
            with jax.named_scope('wait_rows'):
                wait_sib_rows(k)
            for half in range(2):
                span = slice(half * experts * CAP // 2, (half + 1) * experts * CAP // 2)
                xg[span, :] = jnp.dot(gsel[span, :], x_all[k], preferred_element_type=F32).astype(BF16)

            def up_step(e, _):
                q = k * experts + e
                for copy in up_routed(q):
                    copy.wait()
                slot = lax.rem(q + n_shared, UP_SLOTS)
                x = xg[pl.ds(pl.multiple_of(e * CAP, CAP), CAP), :]
                for i, acc in enumerate((acc1, acc3)):
                    d = jnp.dot(x, abuf[slot, i], preferred_element_type=F32)
                    acc[e] = d + jnp.where(k == 0, 0.0, acc[e])

                start_up(q + n_shared + UP_SLOTS)

                for i in range(experts):

                    @pl.when((k == 1) & (e == i))
                    def _():
                        slots = lax.broadcasted_iota(jnp.int32, (total, CAP), 1).astype(F32)
                        hit = slots == jnp.broadcast_to(rank[:, i : i + 1], (total, CAP))
                        ssel[i] = jnp.where(hit, 1.0, 0.0).astype(BF16)
                        wb[i] = jnp.broadcast_to(wmap[:, i : i + 1], (total, 128))

                @pl.when((e == 3) & (k + 1 < K_CHUNKS))
                def _():
                    forward_far(k + 1)

                @pl.when((e == 3) & (k + 2 < K_CHUNKS))
                def _():
                    forward_near(k + 2)

                return 0

            with jax.named_scope('up_steps'):
                lax.fori_loop(0, experts, up_step, 0)

            return 0

        lax.fori_loop(0, K_CHUNKS, up_chunk, 0)

        def activate(e, _):
            inner[e] = (jax.nn.silu(acc1[e]) * acc3[e]).astype(BF16)
            return 0

        with jax.named_scope('act'):
            lax.fori_loop(0, experts, activate, 0)
        for h in range(halves):
            sinner[h] = (jax.nn.silu(sacc1[h]) * sacc3[h]).astype(BF16)
        for i in range(1, n):
            info_copy(i, me, lax.rem(me + i, n)).wait_send()
        for k in range(K_CHUNKS):
            for lane_i in range(7):
                rows_copy(jnp.int32(k), me, lane_i, sib).wait_send()

    def phase_two(ebuf, part, bbuf_hi):
        for e in range(slots):
            down_routed(0, slots + e, bbuf_hi, e, slots + e).start()
        def sib_copy(j, c):
            return remote(
                part.at[j, block(c * 2 + (1 - core))], from_sib.at[j, c], sib_send.at[j, c], sib_recv.at[j, c], sib
            )

        def step_of(j):
            return 1 - 2 * lax.rem(j, 2)

        def tr_copy(j):
            d = step_of(j)
            return remote(part.at[j, block(far)], from_tr.at[j], tr_send.at[j], tr_recv.at[j], dev(chip + d, core))

        def dir_copy(j):
            to = dev(chip - step_of(j), core)
            return remote(part.at[j, block(to)], from_fin.at[1, j], dir_send.at[j], fin_recv.at[1, j], to)

        def com_copy(j):
            to = dev(chip + step_of(j), core)
            return remote(part.at[j, block(to)], from_fin.at[0, j], com_send.at[j], fin_recv.at[0, j], to)

        def products(t, half):
            buf = (bbuf, bbuf_hi)[half]

            def down_step(g, _):
                for u in range(2):
                    slot = g * 2 + u
                    e = half * slots + slot
                    down_routed(t, e, buf, slot, e).wait()
                    d = jnp.dot(inner[e], buf[slot], preferred_element_type=F32)
                    ebuf[t, e] = d.astype(BF16)
                for u in range(2):
                    slot = g * 2 + u
                    e = half * slots + slot

                    @pl.when(t + 1 < N_CHUNKS)
                    def _():
                        down_routed(t + 1, e, buf, slot, e).start()

                    @pl.when(t + 1 == N_CHUNKS)
                    def _():
                        down_shared(e, buf, slot, e).start()

                return 0

            with jax.named_scope('products'):
                lax.fori_loop(0, slots // 2, down_step, 0)

        def spread(t, c):
            span = pl.ds(pl.multiple_of(c * 2 * rows, 32), 2 * rows)
            with jax.named_scope('spread'):
                acc = jnp.zeros((2 * rows, nd), F32)
                for e in range(experts):
                    d = jnp.dot(ssel[e, span, :], ebuf[t, e], preferred_element_type=F32)
                    wt = wb[e, span, :]
                    if nd > 128:
                        wt = jnp.concatenate([wt] * (nd // 128), axis=1)
                    acc = acc + d * wt
                for i in range(per):
                    part[t * per + i, span, :] = acc[:, i * jd : (i + 1) * jd]
            for i in range(per):
                sib_copy(t * per + i, c).start()

        def shared_down(i, half):
            buf = (bbuf, bbuf_hi)[half]
            t = half * (N_CHUNKS // 2) + i
            with jax.named_scope('shared_down'):
                acc = jnp.zeros((rows, nd), F32)
                for h in range(halves):
                    slot = i * halves + h
                    q = half * slots + slot
                    down_shared(q, buf, slot, q).wait()
                    acc = acc + jnp.dot(sinner[h], buf[slot], preferred_element_type=F32)
                for k in range(per):
                    sh[t * per + k] = acc[:, k * jd : (k + 1) * jd]

        def add_sib(t, c):
            with jax.named_scope('add_sib'):
                for i in range(per):
                    j = t * per + i
                    sib_copy(j, c).wait_recv()
                    at = (j, block(c * 2 + core))
                    part[at] = part[at] + from_sib[j, c]

        def near_home(t):
            add_sib(t, chip_right)
            add_sib(t, chip_left)
            for i in range(per):
                dir_copy(t * per + i).start()

        def far_onward(t):
            add_sib(t, chip_far)
            for i in range(per):
                tr_copy(t * per + i).start()

        def far_home(t):
            for i in range(per):
                j = t * per + i
                with jax.named_scope('add_tr'):
                    tr_copy(j).wait_recv()
                    at = (j, block(dev(chip + step_of(j), core)))
                    part[at] = part[at] + from_tr[j]
                com_copy(j).start()

        chip_right, chip_left, chip_far = (lax.rem(chip + i, chips) for i in (1, chips - 1, 2))

        def down_range(t, _):
            products(t, 0)

            @pl.when(t >= 1)
            def _():
                near_home(t - 1)

            products(t, 1)

            def three(i, _):
                spread(t, lax.rem(chip + 2 - i + 3 * (i // 2), chips))
                return 0

            lax.fori_loop(0, 3, three, 0)
            far_onward(t)

            @pl.when(t >= 1)
            def _():
                far_home(t - 1)

            return 0

        lax.fori_loop(0, N_CHUNKS, down_range, 0)
        last = jnp.int32(N_CHUNKS - 1)

        for half in range(2):

            def own_chip(i, _):
                shared_down(i, half)
                if half == 0:

                    @pl.when(i == 0)
                    def _():
                        near_home(last)

                spread(half * (N_CHUNKS // 2) + i, chip)
                return 0

            lax.fori_loop(0, N_CHUNKS // 2, own_chip, 0)
        far_home(last)

        def own_sums(t, _):
            add_sib(t, chip)
            return 0

        lax.fori_loop(0, N_CHUNKS, own_sums, 0)

        for j in range(J_CHUNKS):
            cols = slice(j * jd, (j + 1) * jd)
            with jax.named_scope('home'):
                com_copy(jnp.int32(j)).wait_recv()
                dir_copy(jnp.int32(j)).wait_recv()
            routed = part[j, block(me), :] + (from_fin[0, j] + from_fin[1, j])
            shared_out = sh[j].astype(BF16).astype(F32)
            out_ref[:, cols] = (hid[:, cols].astype(F32) + shared_out + routed).astype(BF16)

        for j in range(J_CHUNKS):
            ji = jnp.int32(j)
            for c in range(chips):
                sib_copy(ji, c).wait_send()
            tr_copy(ji).wait_send()
            dir_copy(ji).wait_send()
            com_copy(ji).wait_send()

    pl.run_scoped(
        phase_one,
        pltpu.VMEM((experts * CAP, kd), BF16),
        pltpu.VMEM((experts * CAP, total), BF16),
        pltpu.VMEM((experts, CAP, ff), F32),
        pltpu.VMEM((experts, CAP, ff), F32),
        pltpu.VMEM((halves, rows, ff), F32),
        pltpu.VMEM((halves, rows, ff), F32),
        pltpu.VMEM((UP_SLOTS, 2, kd, ff), BF16),
    )
    pl.run_scoped(
        phase_two,
        pltpu.VMEM((N_CHUNKS, experts, CAP, nd), BF16),
        pltpu.VMEM((J_CHUNKS, total, jd), F32),
        pltpu.VMEM((slots, ff, nd), BF16),
    )


def routed_layer(n, *args):
    hidden, norm_gain, w_gate, w1_shared, w3_shared, w2_shared, w1_experts, w3_experts, w2_experts, topk_ids = args
    rows, width = hidden.shape
    experts, _, ff = w1_experts.shape
    total = n * rows
    chips = n // 2
    kd = width // K_CHUNKS
    jd = width // J_CHUNKS
    nd = width // N_CHUNKS
    halves = w1_shared.shape[1] // ff
    dma = pltpu.SemaphoreType.DMA
    vmem = pltpu.VMEM
    scratch = [
        vmem((rows, width), BF16),
        vmem((1, width), BF16),
        vmem(w_gate.shape[::-1], BF16),
        vmem(topk_ids.shape[::-1], jnp.int32),
        vmem((128, 128), F32),
        vmem((n, 16, 128), F32),
        vmem((total, 128), F32),
        vmem((total, 128), F32),
        vmem((K_CHUNKS, total, kd), BF16),
        vmem((experts, total, CAP), BF16),
        vmem((experts, total, 128), F32),
        vmem((experts, CAP, ff), BF16),
        vmem((halves, rows, ff), BF16),
        vmem((J_CHUNKS, rows, jd), F32),
        vmem((J_CHUNKS, chips, rows, jd), F32),
        vmem((J_CHUNKS, rows, jd), F32),
        vmem((2, J_CHUNKS, rows, jd), F32),
        vmem((experts // 2, ff, nd), BF16),
        dma((4,)),
        dma((n,)),
        dma((n,)),
        dma((K_CHUNKS, 7)),
        dma((K_CHUNKS, n)),
        dma((UP_SLOTS, 2)),
        dma((experts,)),
        dma((J_CHUNKS, chips)),
        dma((J_CHUNKS, chips)),
        dma((J_CHUNKS,)),
        dma((J_CHUNKS,)),
        dma((J_CHUNKS,)),
        dma((J_CHUNKS,)),
        dma((2, J_CHUNKS)),
    ]
    return pl.pallas_call(
        functools.partial(moe_kernel, n),
        out_shape=[jax.ShapeDtypeStruct((rows, width), BF16), jax.ShapeDtypeStruct((1, 1), jnp.int32)],
        in_specs=[pl.BlockSpec(memory_space=pl.ANY)] * 10,
        out_specs=[pl.BlockSpec(memory_space=pltpu.VMEM), pl.BlockSpec(memory_space=pltpu.SMEM)],
        scratch_shapes=scratch,
        compiler_params=pltpu.CompilerParams(collective_id=0, has_side_effects=True, vmem_limit_bytes=67043328),
        name='moe_layer',
    )(hidden, norm_gain.reshape(1, width), w_gate.T, *args[3:9], topk_ids.T)


def solution(mesh):
    n = mesh.shape['ep']
    tok_spec = P(('dp', 'ep'), None)
    expert_spec = P('ep', None, None)

    def local_fn(*args):
        out, over = routed_layer(n, *args)
        return lax.switch(over[0, 0], (lambda: out, lambda: dense_path(n, *args)))

    return jax.shard_map(local_fn, mesh=mesh, in_specs=(tok_spec, P(), P(), P(), P(), P(), expert_spec, expert_spec, expert_spec, tok_spec), out_specs=tok_spec, check_vma=False)
```

```python
import functools

import jax
import jax.numpy as jnp
from jax import lax
from jax.experimental import pallas as pl
from jax.experimental.pallas import tpu as pltpu
from jax.sharding import PartitionSpec as P

ROUTE_SCALE = 16
NORM_EPS = 1e-6
CAP = 128
K_CHUNKS = 4
J_CHUNKS = 8
N_CHUNKS = 4
UP_SLOTS = 7
EARLY = 4

F32 = jnp.float32
BF16 = jnp.bfloat16


def rms_norm(hidden, norm_gain):
    rows_f = hidden.astype(F32)
    inv_rms = lax.rsqrt(jnp.mean(rows_f * rows_f, axis=-1, keepdims=True) + NORM_EPS)
    return (rows_f * inv_rms * norm_gain.astype(F32)).astype(BF16)


def swiglu(rows_in, w_up, w_lin, w_down):
    gate_act = jnp.dot(rows_in, w_up, preferred_element_type=F32)
    lin_act = jnp.dot(rows_in, w_lin, preferred_element_type=F32)
    inner_act = (jax.nn.silu(gate_act) * lin_act).astype(BF16)
    return jnp.dot(inner_act, w_down, preferred_element_type=F32).astype(BF16)


def dense_path(n, hidden, norm_gain, w_gate, w1_shared, w3_shared, w2_shared, w1_experts, w3_experts, w2_experts, topk_ids):
    normed = rms_norm(hidden, norm_gain)
    probs = jax.nn.softmax(jnp.dot(normed, w_gate, preferred_element_type=F32), axis=-1)
    gate_wts = ROUTE_SCALE * jnp.take_along_axis(probs, topk_ids, axis=1)
    shared_out = swiglu(normed, w1_shared, w3_shared, w2_shared)
    pieces = 4
    width = normed.shape[1] // pieces
    gathered = [
        lax.all_gather(normed[:, i * width : (i + 1) * width], 'ep', axis=0, tiled=True) for i in range(pieces)
    ]
    all_rows = jnp.concatenate(gathered, axis=1)
    all_ids = lax.all_gather(topk_ids, 'ep', axis=0, tiled=True)
    all_wts = lax.all_gather(gate_wts, 'ep', axis=0, tiled=True)
    local_count = w1_experts.shape[0]
    first = lax.axis_index('ep') * local_count

    def one_expert(acc, xs):
        w_up, w_lin, w_down, expert = xs
        column = jnp.sum(jnp.where(all_ids == expert, all_wts, 0.0), axis=1)
        return acc + column[:, None] * swiglu(all_rows, w_up, w_lin, w_down).astype(F32), None

    part, _ = lax.scan(
        one_expert, jnp.zeros(all_rows.shape, F32), (w1_experts, w3_experts, w2_experts, first + jnp.arange(local_count))
    )
    back = lax.all_to_all(part.reshape(n, hidden.shape[0], -1), 'ep', split_axis=0, concat_axis=0)
    return (hidden.astype(F32) + shared_out.astype(F32) + jnp.sum(back, axis=0)).astype(BF16)


def moe_kernel(
    n, hid_hbm, gain_hbm, wg_hbm, w1s, w3s, w2s, w1e, w3e, w2e, ids_hbm,
    out_ref, over_ref,
    hid, gain, wg, ids, tile, info, wmap, rank, x_all, ssel, wb, inner, sacc1, sacc3, sinner, sh,
    from_sib, from_tr, from_fin, bbuf, bbuf_hi, obuf, over,
    in_sem, info_send, info_recv, ag_send, ag_recv, a_sem, s_sem, b_sem,
    sib_send, sib_recv, tr_send, tr_recv, dir_send, com_send, fin_recv, out_sem, over_sem,
):
    rows, width = hid.shape
    experts, _, ff = w1e.shape
    total = n * rows
    chips = n // 2
    kd = width // K_CHUNKS
    jd = width // J_CHUNKS
    nd = width // N_CHUNKS
    per = nd // jd
    halves = w1s.shape[1] // ff
    n_shared = K_CHUNKS * halves
    n_up = K_CHUNKS * experts
    slots = experts // 2
    n_set = K_CHUNKS * slots
    late = n_shared - EARLY

    me = lax.axis_index('ep')
    chip, core = me // 2, lax.rem(me, 2)

    def dev(c, k):
        return lax.rem(c + chips, chips) * 2 + k

    right, left, sib = dev(chip + 1, core), dev(chip - 1, core), dev(chip, 1 - core)
    far = dev(chip + 2, core)

    def block(b):
        return pl.ds(pl.multiple_of(b * rows, 16), rows)

    small = [
        pltpu.make_async_copy(src, dst, in_sem.at[i])
        for i, (src, dst) in enumerate(((hid_hbm, hid), (gain_hbm, gain), (wg_hbm, wg), (ids_hbm, ids)))
    ]
    for copy in small:
        copy.start()

    def down_routed(t, e, buf, slot, sem):
        src = w2e.at[e, :, pl.ds(pl.multiple_of(t * nd, 128), nd)]
        return pltpu.make_async_copy(src, buf.at[slot], b_sem.at[sem])

    def down_shared(q, buf, slot, sem):
        t, h = q // halves, lax.rem(q, halves)
        src = w2s.at[pl.ds(pl.multiple_of(h * ff, 128), ff), pl.ds(pl.multiple_of(t * nd, 128), nd)]
        return pltpu.make_async_copy(src, buf.at[slot], b_sem.at[sem])

    barrier = pltpu.get_barrier_semaphore()
    for i in range(1, n):
        pl.semaphore_signal(
            barrier, inc=1, device_id={'ep': lax.rem(me + i, n)}, device_id_type=pl.DeviceIdType.MESH
        )

    def remote(src, dst, send, recv, to):
        return pltpu.make_async_remote_copy(
            src_ref=src, dst_ref=dst, send_sem=send, recv_sem=recv, device_id={'ep': to}, device_id_type=pl.DeviceIdType.MESH
        )

    def shared_src(s):
        k, h = s // halves, lax.rem(s, halves)
        at = (pl.ds(pl.multiple_of(k * kd, 128), kd), pl.ds(pl.multiple_of(h * ff, 128), ff))
        return w1s.at[at], w3s.at[at]

    def two_products(buf, x, slot, put):
        cut = ff // 256 * 256
        put(0, slice(0, cut), jnp.dot(x, buf[slot, 0, :, 0:cut], preferred_element_type=F32))
        put(1, slice(0, cut), jnp.dot(x, buf[slot, 1, :, 0:cut], preferred_element_type=F32))
        if cut < ff:
            rest = jnp.concatenate([buf[slot, 0, :, cut:ff], buf[slot, 1, :, cut:ff]], axis=1)
            d = jnp.dot(x, rest, preferred_element_type=F32)
            put(0, slice(cut, ff), d[:, : ff - cut])
            put(1, slice(cut, ff), d[:, ff - cut :])

    def shared_product(s, buf, slot):
        k, h = s // halves, lax.rem(s, halves)

        def put(i, cols, d):
            acc = (sacc1, sacc3)[i]
            acc[h, :, cols] = d + jnp.where(k == 0, 0.0, acc[h, :, cols])

        two_products(buf, x_all[k, block(me), :], slot, put)

    def late_copies(i, sbuf):
        return [
            pltpu.make_async_copy(src, sbuf.at[i, m], s_sem.at[i, m])
            for m, src in enumerate(shared_src(jnp.int32(EARLY) + i))
        ]

    def late_shared(i, sbuf):
        for copy in late_copies(i, sbuf):
            copy.start()

    over_copy = pltpu.make_async_copy(over, over_ref, over_sem)

    def phase_one(xg, gsel, acc1, acc3, abuf):
        def up_pair(pair, slot):
            return [pltpu.make_async_copy(src, abuf.at[slot, i], a_sem.at[slot, i]) for i, src in enumerate(pair)]

        def up_shared(s):
            return up_pair(shared_src(s), lax.rem(s, UP_SLOTS))

        def up_routed(q):
            k, e = lax.rem(q // slots, K_CHUNKS), q // n_set * slots + lax.rem(q, slots)
            at = (e, pl.ds(pl.multiple_of(k * kd, 128), kd))
            return up_pair((w1e.at[at], w3e.at[at]), lax.rem(q + EARLY, UP_SLOTS))

        def start_up(s):
            @pl.when(s < EARLY)
            def _():
                for copy in up_shared(s):
                    copy.start()

            @pl.when((s >= EARLY) & (s < EARLY + n_up))
            def _():
                for copy in up_routed(s - EARLY):
                    copy.start()

        with jax.named_scope('small_in'):
            for copy in small:
                copy.wait()
        for s in range(UP_SLOTS):
            start_up(jnp.int32(s))
        for e in range(experts // 2):
            down_routed(0, e, bbuf, e, e).start()
        for e in range(experts // 2):
            down_routed(0, slots + e, bbuf_hi, e, slots + e).start()
        with jax.named_scope('norm'):
            rows_f = hid[...].astype(F32)
            inv_rms = lax.rsqrt(jnp.mean(rows_f * rows_f, axis=-1, keepdims=True) + NORM_EPS)
            for i in range(width // 128):
                piece = rows_f[:, i * 128 : (i + 1) * 128] * inv_rms * gain[i : i + 1, :].astype(F32)
                off = i * 128 % kd
                x_all[i * 128 // kd, block(me), off : off + 128] = piece.astype(BF16)
        with jax.named_scope('barrier'):
            pl.semaphore_wait(barrier, n - 1)

        def rows_copy(k, b, lane, to):
            at = (k, block(b))
            return remote(x_all.at[at], x_all.at[at], ag_send.at[k, lane], ag_recv.at[k, b], to)

        def send_own(k):
            rows_copy(k, me, 0, right).start()
            rows_copy(k, me, 1, left).start()
            rows_copy(k, me, 2, sib).start()

        def forward_near(k):
            rows_copy(k, left, 3, sib).wait_recv()
            rows_copy(k, right, 4, sib).wait_recv()
            even = lax.rem(k, 2) == 0
            onward = jnp.where(even, left, right)
            to = jnp.where(even, right, left)
            rows_copy(k, onward, 5, to).start()
            rows_copy(k, left, 3, sib).start()
            rows_copy(k, right, 4, sib).start()

        def forward_far(k):
            rows_copy(k, far, 6, sib).wait_recv()
            rows_copy(k, far, 6, sib).start()

        def wait_sib_rows(k):
            for i in range(chips):
                rows_copy(k, dev(chip + i, 1 - core), 0, sib).wait_recv()

        send_own(0)

        logits = jnp.concatenate([x_all[k, block(me), :] for k in range(K_CHUNKS)], axis=1)
        logits = lax.dot_general(logits, wg[...], (((1,), (1,)), ((), ())), preferred_element_type=F32)
        expd = jnp.exp(logits - jnp.max(logits, axis=-1, keepdims=True))
        probs = expd / jnp.sum(expd, axis=-1, keepdims=True)
        top_k = ids.shape[0]
        tile[...] = jnp.zeros_like(tile)
        tile[0:top_k, 0:rows] = ids[...].astype(F32)
        id_cols = tile[...].T[0:rows, :]
        expert_lane = lax.broadcasted_iota(jnp.int32, probs.shape, 1).astype(F32)
        lane = lax.broadcasted_iota(jnp.int32, (rows, 128), 1)
        packed = jnp.zeros((rows, 128), F32)
        for i in range(top_k):
            col = id_cols[:, i : i + 1]
            wt = ROUTE_SCALE * jnp.sum(jnp.where(expert_lane == col, probs, 0.0), axis=-1, keepdims=True)
            packed = jnp.where(lane == i, wt, packed)
            packed = jnp.where(lane == 8 + i, col, packed)
        tile[...] = jnp.zeros_like(tile)
        tile[0:rows, :] = packed
        info[me] = tile[...].T[0:16, :]

        def info_copy(i, b, to):
            return remote(info.at[b], info.at[b], info_send.at[i], info_recv.at[b], to)

        for i in range(1, n):
            info_copy(i, me, lax.rem(me + i, n)).start()
        send_own(1)

        def shared_step(s, _):
            for copy in up_shared(s):
                copy.wait()
            shared_product(s, abuf, lax.rem(s, UP_SLOTS))
            start_up(s + UP_SLOTS)
            return 0

        def shared_steps(first_s, last_s):
            with jax.named_scope('shared_up'):
                lax.fori_loop(first_s, last_s, shared_step, 0)

        def tables():
            for i in range(1, n):
                b = lax.rem(me + i, n)
                info_copy(i, b, b).wait_recv()
            info_cols = info[...].reshape(n * 16, 128).T
            first = (me * experts).astype(F32)
            all_experts = float(n * experts)
            lane_f = lax.broadcasted_iota(jnp.int32, (rows, 128), 1).astype(F32)
            lower = lax.broadcasted_iota(jnp.int32, (rows, rows), 0) > lax.broadcasted_iota(jnp.int32, (rows, rows), 1)
            lower = jnp.where(lower, 1.0, 0.0).astype(BF16)
            seen = jnp.zeros((1, 128), F32)
            for b in range(n):
                wm = jnp.zeros((rows, 128), F32)
                hit_any = jnp.zeros((rows, 128), F32)
                for i in range(top_k):
                    wt = info_cols[0:rows, 16 * b + i : 16 * b + i + 1]
                    at = info_cols[0:rows, 16 * b + 8 + i : 16 * b + 9 + i] - first
                    at = jnp.where(at < 0, at + all_experts, at)
                    hit = lane_f == at
                    wm = jnp.where(hit, wt, wm)
                    hit_any = jnp.where(hit, 1.0, hit_any)
                before = jnp.dot(lower, hit_any.astype(BF16), preferred_element_type=F32) + seen
                wmap[b * rows : (b + 1) * rows, :] = wm
                rank[b * rows : (b + 1) * rows, :] = jnp.where(hit_any > 0, before, -1.0)
                seen = seen + jnp.sum(hit_any, axis=0, keepdims=True)
            over[0, 0] = (jnp.max(seen) > CAP).astype(jnp.int32)
            over_copy.start()
            rank_rows = rank[...].T
            place = lax.broadcasted_iota(jnp.int32, (CAP, total), 0).astype(F32)
            for e in range(experts):
                hit = place == jnp.broadcast_to(rank_rows[e : e + 1, :], (CAP, total))
                gsel[e * CAP : (e + 1) * CAP, :] = jnp.where(hit, 1.0, 0.0).astype(BF16)

        shared_steps(0, EARLY)
        with jax.named_scope('near0'):
            forward_near(jnp.int32(0))
            send_own(jnp.int32(2))
        with jax.named_scope('info'):
            tables()
        with jax.named_scope('near1'):
            forward_near(jnp.int32(1))
            send_own(jnp.int32(3))
        with jax.named_scope('select'):
            place_lane = lax.broadcasted_iota(jnp.int32, (total, CAP), 1).astype(F32)
            for e in range(experts):
                hit = place_lane == jnp.broadcast_to(rank[:, e : e + 1], (total, CAP))
                ssel[e] = jnp.where(hit, 1.0, 0.0).astype(BF16)
                wb[e] = jnp.broadcast_to(wmap[:, e : e + 1], (total, 128))
        with jax.named_scope('far0'):
            forward_far(jnp.int32(0))

        def up_chunk(kk, _):
            k, base = lax.rem(kk, K_CHUNKS), kk // K_CHUNKS * slots

            @pl.when(kk < K_CHUNKS)
            def _():
                with jax.named_scope('wait_rows'):
                    wait_sib_rows(k)

            with jax.named_scope('gather'):
                span = pl.ds(pl.multiple_of(base * CAP, CAP), slots * CAP)
                xg[...] = jnp.dot(gsel[span, :], x_all[k], preferred_element_type=F32).astype(BF16)

            def up_step(g, _):
                for u in range(2):
                    for copy in up_routed(kk * slots + g * 2 + u):
                        copy.wait()
                for u in range(2):
                    i_e = g * 2 + u

                    def put(i, cols, d):
                        acc = (acc1, acc3)[i]
                        acc[i_e, :, cols] = d + jnp.where(k == 0, 0.0, acc[i_e, :, cols])

                    two_products(
                        abuf,
                        xg[pl.ds(pl.multiple_of(i_e * CAP, CAP), CAP), :],
                        lax.rem(kk * slots + i_e + EARLY, UP_SLOTS),
                        put,
                    )
                for u in range(2):
                    start_up(kk * slots + g * 2 + u + EARLY + UP_SLOTS)

                @pl.when((g == 1) & (kk + 1 < K_CHUNKS))
                def _():
                    forward_far(kk + 1)

                @pl.when((g == 0) & (kk + 2 < K_CHUNKS))
                def _():
                    forward_near(kk + 2)

                @pl.when(k == K_CHUNKS - 1)
                def _():
                    for u in range(2):
                        i_e = g * 2 + u
                        inner[base + i_e] = (jax.nn.silu(acc1[i_e]) * acc3[i_e]).astype(BF16)

                return 0

            with jax.named_scope('up_steps'):
                lax.fori_loop(0, slots // 2, up_step, 0)

            return 0

        lax.fori_loop(0, 2 * K_CHUNKS, up_chunk, 0)
        for i in range(1, n):
            info_copy(i, me, lax.rem(me + i, n)).wait_send()
        for k in range(K_CHUNKS):
            for lane_i in range(7):
                rows_copy(jnp.int32(k), me, lane_i, sib).wait_send()

    def phase_two(ebuf, part, sbuf):
        late_shared(0, sbuf)
        def sib_copy(j, c):
            return remote(
                part.at[j, block(c * 2 + (1 - core))], from_sib.at[j, c], sib_send.at[j, c], sib_recv.at[j, c], sib
            )

        def step_of(j):
            return 1 - 2 * lax.rem(j, 2)

        def tr_copy(j):
            d = step_of(j)
            return remote(part.at[j, block(far)], from_tr.at[j], tr_send.at[j], tr_recv.at[j], dev(chip + d, core))

        def dir_copy(j):
            to = dev(chip - step_of(j), core)
            return remote(part.at[j, block(to)], from_fin.at[1, j], dir_send.at[j], fin_recv.at[1, j], to)

        def com_copy(j):
            to = dev(chip + step_of(j), core)
            return remote(part.at[j, block(to)], from_fin.at[0, j], com_send.at[j], fin_recv.at[0, j], to)

        def products(t, half):
            buf = (bbuf, bbuf_hi)[half]
            with jax.named_scope('products'):
                for slot in range(slots):
                    e = half * slots + slot
                    down_routed(t, e, buf, slot, e).wait()
                for slot in range(slots):
                    e = half * slots + slot
                    d = jnp.dot(inner[e], buf[slot], preferred_element_type=F32)
                    ebuf[t, e] = d.astype(BF16)

                @pl.when(t + 1 < N_CHUNKS)
                def _():
                    for slot in range(slots):
                        e = half * slots + slot
                        down_routed(t + 1, e, buf, slot, e).start()

                @pl.when(t + 1 == N_CHUNKS)
                def _():
                    for slot in range(slots):
                        e = half * slots + slot
                        down_shared(e, buf, slot, e).start()

        def spread(t, c):
            span = pl.ds(pl.multiple_of(c * 2 * rows, 32), 2 * rows)
            with jax.named_scope('spread'):
                acc = jnp.zeros((2 * rows, nd), F32)
                for e in range(experts):
                    d = jnp.dot(ssel[e, span, :], ebuf[t, e], preferred_element_type=F32)
                    wt = wb[e, span, :]
                    if nd > 128:
                        wt = jnp.concatenate([wt] * (nd // 128), axis=1)
                    acc = acc + d * wt
                for i in range(per):
                    part[t * per + i, span, :] = acc[:, i * jd : (i + 1) * jd]
            for i in range(per):
                sib_copy(t * per + i, c).start()

        def shared_down(i, half):
            buf = (bbuf, bbuf_hi)[half]
            t = half * (N_CHUNKS // 2) + i
            with jax.named_scope('shared_down'):
                acc = jnp.zeros((rows, nd), F32)
                for h in range(halves):
                    slot = i * halves + h
                    q = half * slots + slot
                    down_shared(q, buf, slot, q).wait()
                    acc = acc + jnp.dot(sinner[h], buf[slot], preferred_element_type=F32)
                for k in range(per):
                    sh[t * per + k] = acc[:, k * jd : (k + 1) * jd]

        def add_sib(t, c):
            with jax.named_scope('add_sib'):
                for i in range(per):
                    j = t * per + i
                    sib_copy(j, c).wait_recv()
                    at = (j, block(c * 2 + core))
                    part[at] = part[at] + from_sib[j, c]

        def near_home(t):
            add_sib(t, chip_right)
            add_sib(t, chip_left)
            for i in range(per):
                dir_copy(t * per + i).start()

        def far_onward(t):
            add_sib(t, chip_far)
            for i in range(per):
                tr_copy(t * per + i).start()

        def far_home(t):
            for i in range(per):
                j = t * per + i
                with jax.named_scope('add_tr'):
                    tr_copy(j).wait_recv()
                    at = (j, block(dev(chip + step_of(j), core)))
                    part[at] = part[at] + from_tr[j]
                com_copy(j).start()

        chip_right, chip_left, chip_far = (lax.rem(chip + i, chips) for i in (1, chips - 1, 2))

        def down_range(t, _):
            products(t, 0)

            @pl.when(t >= 1)
            def _():
                near_home(t - 1)

            products(t, 1)

            spread(t, chip_far)

            def near(i, _):
                spread(t, lax.rem(chip + 1 + 2 * i, chips))
                return 0

            lax.fori_loop(0, 2, near, 0)
            far_onward(t)

            @pl.when(t + 1 < late)
            def _():
                late_shared(t + 1, sbuf)

            with jax.named_scope('late_shared'):
                for copy in late_copies(t, sbuf):
                    copy.wait()
                shared_product(EARLY + t, sbuf, t)

            @pl.when(t >= 1)
            def _():
                far_home(t - 1)

            return 0

        lax.fori_loop(0, N_CHUNKS, down_range, 0)
        last = jnp.int32(N_CHUNKS - 1)
        for h in range(halves):
            sinner[h] = (jax.nn.silu(sacc1[h]) * sacc3[h]).astype(BF16)

        for half in range(2):

            def own_chip(i, _):
                shared_down(i, half)
                if half == 0:

                    @pl.when(i == 0)
                    def _():
                        near_home(last)

                spread(half * (N_CHUNKS // 2) + i, chip)
                return 0

            lax.fori_loop(0, N_CHUNKS // 2, own_chip, 0)
        far_home(last)

        def own_sums(t, _):
            add_sib(t, chip)
            return 0

        lax.fori_loop(0, N_CHUNKS, own_sums, 0)

        for j in range(J_CHUNKS):
            cols = slice(j * jd, (j + 1) * jd)
            with jax.named_scope('home'):
                com_copy(jnp.int32(j)).wait_recv()
                dir_copy(jnp.int32(j)).wait_recv()
            routed = part[j, block(me), :] + (from_fin[0, j] + from_fin[1, j])
            shared_out = sh[j].astype(BF16).astype(F32)
            obuf[:, cols] = (hid[:, cols].astype(F32) + shared_out + routed).astype(BF16)
            pltpu.make_async_copy(obuf.at[:, cols], out_ref.at[:, cols], out_sem.at[j]).start()

        with jax.named_scope('sent'):
            over_copy.wait()
            for j in range(J_CHUNKS):
                ji = jnp.int32(j)
                for c in range(chips):
                    sib_copy(ji, c).wait_send()
                tr_copy(ji).wait_send()
                dir_copy(ji).wait_send()
                com_copy(ji).wait_send()
            for j in range(J_CHUNKS):
                cols = slice(j * jd, (j + 1) * jd)
                pltpu.make_async_copy(obuf.at[:, cols], out_ref.at[:, cols], out_sem.at[j]).wait()

    pl.run_scoped(
        phase_one,
        pltpu.VMEM((experts // 2 * CAP, kd), BF16),
        pltpu.VMEM((experts * CAP, total), BF16),
        pltpu.VMEM((experts // 2, CAP, ff), F32),
        pltpu.VMEM((experts // 2, CAP, ff), F32),
        pltpu.VMEM((UP_SLOTS, 2, kd, ff), BF16),
    )
    pl.run_scoped(
        phase_two,
        pltpu.VMEM((N_CHUNKS, experts, CAP, nd), BF16),
        pltpu.VMEM((J_CHUNKS, total, jd), F32),
        pltpu.VMEM((late, 2, kd, ff), BF16),
    )


def routed_layer(n, *args):
    hidden, norm_gain, w_gate, w1_shared, w3_shared, w2_shared, w1_experts, w3_experts, w2_experts, topk_ids = args
    rows, width = hidden.shape
    experts, _, ff = w1_experts.shape
    total = n * rows
    chips = n // 2
    kd = width // K_CHUNKS
    jd = width // J_CHUNKS
    nd = width // N_CHUNKS
    halves = w1_shared.shape[1] // ff
    dma = pltpu.SemaphoreType.DMA
    vmem = pltpu.VMEM
    scratch = [
        vmem((rows, width), BF16),
        vmem((width // 128, 128), BF16),
        vmem(w_gate.shape[::-1], BF16),
        vmem(topk_ids.shape[::-1], jnp.int32),
        vmem((128, 128), F32),
        vmem((n, 16, 128), F32),
        vmem((total, 128), F32),
        vmem((total, 128), F32),
        vmem((K_CHUNKS, total, kd), BF16),
        vmem((experts, total, CAP), BF16),
        vmem((experts, total, 128), F32),
        vmem((experts, CAP, ff), BF16),
        vmem((halves, rows, ff), F32),
        vmem((halves, rows, ff), F32),
        vmem((halves, rows, ff), BF16),
        vmem((J_CHUNKS, rows, jd), F32),
        vmem((J_CHUNKS, chips, rows, jd), F32),
        vmem((J_CHUNKS, rows, jd), F32),
        vmem((2, J_CHUNKS, rows, jd), F32),
        vmem((experts // 2, ff, nd), BF16),
        vmem((experts // 2, ff, nd), BF16),
        vmem((rows, width), BF16),
        pltpu.SMEM((1, 1), jnp.int32),
        dma((4,)),
        dma((n,)),
        dma((n,)),
        dma((K_CHUNKS, 7)),
        dma((K_CHUNKS, n)),
        dma((UP_SLOTS, 2)),
        dma((K_CHUNKS * halves - EARLY, 2)),
        dma((experts,)),
        dma((J_CHUNKS, chips)),
        dma((J_CHUNKS, chips)),
        dma((J_CHUNKS,)),
        dma((J_CHUNKS,)),
        dma((J_CHUNKS,)),
        dma((J_CHUNKS,)),
        dma((2, J_CHUNKS)),
        dma((J_CHUNKS,)),
        dma(()),
    ]
    return pl.pallas_call(
        functools.partial(moe_kernel, n),
        out_shape=[jax.ShapeDtypeStruct((rows, width), BF16), jax.ShapeDtypeStruct((1, 1), jnp.int32)],
        in_specs=[pl.BlockSpec(memory_space=pl.ANY)] * 10,
        out_specs=[pl.BlockSpec(memory_space=pl.ANY), pl.BlockSpec(memory_space=pl.ANY)],
        scratch_shapes=scratch,
        compiler_params=pltpu.CompilerParams(collective_id=0, has_side_effects=True, vmem_limit_bytes=67043328),
        name='moe_layer',
    )(hidden, norm_gain.reshape(-1, 128), w_gate.T, *args[3:9], topk_ids.T)


def solution(mesh):
    n = mesh.shape['ep']
    tok_spec = P(('dp', 'ep'), None)
    expert_spec = P('ep', None, None)

    def local_fn(*args):
        out, over = routed_layer(n, *args)
        return lax.switch(over[0, 0], (lambda: out, lambda: dense_path(n, *args)))

    return jax.shard_map(local_fn, mesh=mesh, in_specs=(tok_spec, P(), P(), P(), P(), P(), expert_spec, expert_spec, expert_spec, tok_spec), out_specs=tok_spec, check_vma=False)
```

```python
import functools

import jax
import jax.numpy as jnp
from jax import lax
from jax.experimental import pallas as pl
from jax.experimental.pallas import tpu as pltpu
from jax.sharding import PartitionSpec as P

ROUTE_SCALE = 16
NORM_EPS = 1e-6
CAP = 128
K_CHUNKS = 4
J_CHUNKS = 8
N_CHUNKS = 4
UP_SLOTS = 7
LATE_SLOTS = 4

F32 = jnp.float32
BF16 = jnp.bfloat16


def rms_norm(hidden, norm_gain):
    rows_f = hidden.astype(F32)
    inv_rms = lax.rsqrt(jnp.mean(rows_f * rows_f, axis=-1, keepdims=True) + NORM_EPS)
    return (rows_f * inv_rms * norm_gain.astype(F32)).astype(BF16)


def swiglu(rows_in, w_up, w_lin, w_down):
    gate_act = jnp.dot(rows_in, w_up, preferred_element_type=F32)
    lin_act = jnp.dot(rows_in, w_lin, preferred_element_type=F32)
    inner_act = (jax.nn.silu(gate_act) * lin_act).astype(BF16)
    return jnp.dot(inner_act, w_down, preferred_element_type=F32).astype(BF16)


def dense_path(n, hidden, norm_gain, w_gate, w1_shared, w3_shared, w2_shared, w1_experts, w3_experts, w2_experts, topk_ids):
    normed = rms_norm(hidden, norm_gain)
    probs = jax.nn.softmax(jnp.dot(normed, w_gate, preferred_element_type=F32), axis=-1)
    gate_wts = ROUTE_SCALE * jnp.take_along_axis(probs, topk_ids, axis=1)
    shared_out = swiglu(normed, w1_shared, w3_shared, w2_shared)
    pieces = 4
    width = normed.shape[1] // pieces
    gathered = [
        lax.all_gather(normed[:, i * width : (i + 1) * width], 'ep', axis=0, tiled=True) for i in range(pieces)
    ]
    all_rows = jnp.concatenate(gathered, axis=1)
    all_ids = lax.all_gather(topk_ids, 'ep', axis=0, tiled=True)
    all_wts = lax.all_gather(gate_wts, 'ep', axis=0, tiled=True)
    local_count = w1_experts.shape[0]
    first = lax.axis_index('ep') * local_count

    def one_expert(acc, xs):
        w_up, w_lin, w_down, expert = xs
        column = jnp.sum(jnp.where(all_ids == expert, all_wts, 0.0), axis=1)
        return acc + column[:, None] * swiglu(all_rows, w_up, w_lin, w_down).astype(F32), None

    part, _ = lax.scan(
        one_expert, jnp.zeros(all_rows.shape, F32), (w1_experts, w3_experts, w2_experts, first + jnp.arange(local_count))
    )
    back = lax.all_to_all(part.reshape(n, hidden.shape[0], -1), 'ep', split_axis=0, concat_axis=0)
    return (hidden.astype(F32) + shared_out.astype(F32) + jnp.sum(back, axis=0)).astype(BF16)


def moe_kernel(
    n, hid_hbm, gain_hbm, wg_hbm, w1s, w3s, w2s, w1e, w3e, w2e, ids_hbm,
    out_ref, over_ref,
    hid, gain, wg, ids, tile, info, wmap, rank, x_all, ssel, wb, inner,
    from_sib, from_tr, from_fin, bbuf, bbuf_hi, over,
    in_sem, info_send, info_recv, ag_send, ag_recv, a_sem, s_sem, b_sem,
    sib_send, sib_recv, tr_send, tr_recv, dir_send, com_send, fin_recv, out_sem, over_sem,
):
    rows, width = hid.shape
    experts, _, ff = w1e.shape
    total = n * rows
    chips = n // 2
    kd = width // K_CHUNKS
    jd = width // J_CHUNKS
    nd = width // N_CHUNKS
    per = nd // jd
    halves = w1s.shape[1] // ff
    n_shared = K_CHUNKS * halves
    n_up = K_CHUNKS * experts
    slots = experts // 2
    turn = n_shared // N_CHUNKS

    me = lax.axis_index('ep')
    chip, core = me // 2, lax.rem(me, 2)

    def dev(c, k):
        return lax.rem(c + chips, chips) * 2 + k

    right, left, sib = dev(chip + 1, core), dev(chip - 1, core), dev(chip, 1 - core)
    far = dev(chip + 2, core)

    def block(b):
        return pl.ds(pl.multiple_of(b * rows, 16), rows)

    small = [
        pltpu.make_async_copy(src, dst, in_sem.at[i])
        for i, (src, dst) in enumerate(((hid_hbm, hid), (gain_hbm, gain), (wg_hbm, wg), (ids_hbm, ids)))
    ]
    for copy in small:
        copy.start()

    def down_routed(t, e, buf, slot, sem):
        src = w2e.at[e, :, pl.ds(pl.multiple_of(t * nd, 128), nd)]
        return pltpu.make_async_copy(src, buf.at[slot], b_sem.at[sem])

    def down_shared(q, buf, slot, sem):
        t, h = q // halves, lax.rem(q, halves)
        src = w2s.at[pl.ds(pl.multiple_of(h * ff, 128), ff), pl.ds(pl.multiple_of(t * nd, 128), nd)]
        return pltpu.make_async_copy(src, buf.at[slot], b_sem.at[sem])

    barrier = pltpu.get_barrier_semaphore()
    for i in range(1, n):
        pl.semaphore_signal(
            barrier, inc=1, device_id={'ep': lax.rem(me + i, n)}, device_id_type=pl.DeviceIdType.MESH
        )

    def remote(src, dst, send, recv, to):
        return pltpu.make_async_remote_copy(
            src_ref=src, dst_ref=dst, send_sem=send, recv_sem=recv, device_id={'ep': to}, device_id_type=pl.DeviceIdType.MESH
        )

    def shared_src(s):
        k, h = s // halves, lax.rem(s, halves)
        at = (pl.ds(pl.multiple_of(k * kd, 128), kd), pl.ds(pl.multiple_of(h * ff, 128), ff))
        return w1s.at[at], w3s.at[at]

    def two_products(buf, x, slot, put):
        cut = ff // 256 * 256
        put(0, slice(0, cut), jnp.dot(x, buf[slot, 0, :, 0:cut], preferred_element_type=F32))
        put(1, slice(0, cut), jnp.dot(x, buf[slot, 1, :, 0:cut], preferred_element_type=F32))
        if cut < ff:
            rest = jnp.concatenate([buf[slot, 0, :, cut:ff], buf[slot, 1, :, cut:ff]], axis=1)
            d = jnp.dot(x, rest, preferred_element_type=F32)
            put(0, slice(cut, ff), d[:, : ff - cut])
            put(1, slice(cut, ff), d[:, ff - cut :])

    over_copy = pltpu.make_async_copy(over, over_ref, over_sem)

    def phase_one(xg, gsel, acc1, acc3, abuf):
        def up_pair(pair, slot):
            return [pltpu.make_async_copy(src, abuf.at[slot, i], a_sem.at[slot, i]) for i, src in enumerate(pair)]

        def up_routed(q):
            k, e = q // experts, lax.rem(q, experts)
            at = (e, pl.ds(pl.multiple_of(k * kd, 128), kd))
            return up_pair((w1e.at[at], w3e.at[at]), lax.rem(q, UP_SLOTS))

        def start_up(q):
            @pl.when(q < n_up)
            def _():
                for copy in up_routed(q):
                    copy.start()

        with jax.named_scope('small_in'):
            for copy in small:
                copy.wait()
        for s in range(UP_SLOTS):
            start_up(jnp.int32(s))
        for e in range(experts // 2):
            down_routed(0, e, bbuf, e, e).start()
        for e in range(experts // 2):
            down_routed(0, slots + e, bbuf_hi, e, slots + e).start()
        with jax.named_scope('norm'):
            rows_f = hid[...].astype(F32)
            inv_rms = lax.rsqrt(jnp.mean(rows_f * rows_f, axis=-1, keepdims=True) + NORM_EPS)
            for i in range(width // 128):
                piece = rows_f[:, i * 128 : (i + 1) * 128] * inv_rms * gain[i : i + 1, :].astype(F32)
                off = i * 128 % kd
                x_all[i * 128 // kd, block(me), off : off + 128] = piece.astype(BF16)
        with jax.named_scope('barrier'):
            pl.semaphore_wait(barrier, n - 1)

        def rows_copy(k, b, lane, to):
            at = (k, block(b))
            return remote(x_all.at[at], x_all.at[at], ag_send.at[k, lane], ag_recv.at[k, b], to)

        def send_own(k):
            rows_copy(k, me, 0, right).start()
            rows_copy(k, me, 1, left).start()
            rows_copy(k, me, 2, sib).start()

        def forward_near(k):
            rows_copy(k, left, 3, sib).wait_recv()
            rows_copy(k, right, 4, sib).wait_recv()
            even = lax.rem(k, 2) == 0
            onward = jnp.where(even, left, right)
            to = jnp.where(even, right, left)
            rows_copy(k, onward, 5, to).start()
            rows_copy(k, left, 3, sib).start()
            rows_copy(k, right, 4, sib).start()

        def forward_far(k):
            rows_copy(k, far, 6, sib).wait_recv()
            rows_copy(k, far, 6, sib).start()

        def wait_sib_rows(k):
            for i in range(chips):
                rows_copy(k, dev(chip + i, 1 - core), 0, sib).wait_recv()

        send_own(0)

        logits = jnp.concatenate([x_all[k, block(me), :] for k in range(K_CHUNKS)], axis=1)
        logits = lax.dot_general(logits, wg[...], (((1,), (1,)), ((), ())), preferred_element_type=F32)
        expd = jnp.exp(logits - jnp.max(logits, axis=-1, keepdims=True))
        probs = expd / jnp.sum(expd, axis=-1, keepdims=True)
        top_k = ids.shape[0]
        tile[...] = jnp.zeros_like(tile)
        tile[0:top_k, 0:rows] = ids[...].astype(F32)
        id_cols = tile[...].T[0:rows, :]
        expert_lane = lax.broadcasted_iota(jnp.int32, probs.shape, 1).astype(F32)
        lane = lax.broadcasted_iota(jnp.int32, (rows, 128), 1)
        packed = jnp.zeros((rows, 128), F32)
        for i in range(top_k):
            col = id_cols[:, i : i + 1]
            wt = ROUTE_SCALE * jnp.sum(jnp.where(expert_lane == col, probs, 0.0), axis=-1, keepdims=True)
            packed = jnp.where(lane == i, wt, packed)
            packed = jnp.where(lane == 8 + i, col, packed)
        tile[...] = jnp.zeros_like(tile)
        tile[0:rows, :] = packed
        info[me] = tile[...].T[0:16, :]

        def info_copy(i, b, to):
            return remote(info.at[b], info.at[b], info_send.at[i], info_recv.at[b], to)

        for i in range(1, n):
            info_copy(i, me, lax.rem(me + i, n)).start()
        send_own(1)

        def tables():
            for i in range(1, n):
                b = lax.rem(me + i, n)
                info_copy(i, b, b).wait_recv()
            info_cols = info[...].reshape(n * 16, 128).T
            first = (me * experts).astype(F32)
            all_experts = float(n * experts)
            lane_f = lax.broadcasted_iota(jnp.int32, (rows, 128), 1).astype(F32)
            lower = lax.broadcasted_iota(jnp.int32, (rows, rows), 0) > lax.broadcasted_iota(jnp.int32, (rows, rows), 1)
            lower = jnp.where(lower, 1.0, 0.0).astype(BF16)
            seen = jnp.zeros((1, 128), F32)
            for b in range(n):
                wm = jnp.zeros((rows, 128), F32)
                hit_any = jnp.zeros((rows, 128), F32)
                for i in range(top_k):
                    wt = info_cols[0:rows, 16 * b + i : 16 * b + i + 1]
                    at = info_cols[0:rows, 16 * b + 8 + i : 16 * b + 9 + i] - first
                    at = jnp.where(at < 0, at + all_experts, at)
                    hit = lane_f == at
                    wm = jnp.where(hit, wt, wm)
                    hit_any = jnp.where(hit, 1.0, hit_any)
                before = jnp.dot(lower, hit_any.astype(BF16), preferred_element_type=F32) + seen
                wmap[b * rows : (b + 1) * rows, :] = wm
                rank[b * rows : (b + 1) * rows, :] = jnp.where(hit_any > 0, before, -1.0)
                seen = seen + jnp.sum(hit_any, axis=0, keepdims=True)
            over[0, 0] = (jnp.max(seen) > CAP).astype(jnp.int32)
            over_copy.start()
            rank_rows = rank[...].T
            place = lax.broadcasted_iota(jnp.int32, (CAP, total), 0).astype(F32)
            for e in range(experts):
                hit = place == jnp.broadcast_to(rank_rows[e : e + 1, :], (CAP, total))
                gsel[e * CAP : (e + 1) * CAP, :] = jnp.where(hit, 1.0, 0.0).astype(BF16)

        with jax.named_scope('near0'):
            forward_near(jnp.int32(0))
            send_own(jnp.int32(2))
        with jax.named_scope('info'):
            tables()
        with jax.named_scope('near1'):
            forward_near(jnp.int32(1))
            send_own(jnp.int32(3))
        with jax.named_scope('select'):
            place_lane = lax.broadcasted_iota(jnp.int32, (total, CAP), 1).astype(F32)
            for e in range(experts):
                hit = place_lane == jnp.broadcast_to(rank[:, e : e + 1], (total, CAP))
                ssel[e] = jnp.where(hit, 1.0, 0.0).astype(BF16)
                wb[e] = jnp.broadcast_to(wmap[:, e : e + 1], (total, 128))
        with jax.named_scope('far0'):
            forward_far(jnp.int32(0))

        def up_chunk(k, last):
            with jax.named_scope('wait_rows'):
                wait_sib_rows(k)
            with jax.named_scope('gather'):
                for half in range(2):
                    span = slice(half * experts * CAP // 2, (half + 1) * experts * CAP // 2)
                    xg[span, :] = jnp.dot(gsel[span, :], x_all[k], preferred_element_type=F32).astype(BF16)

            def up_step(g, _):
                for u in range(2):
                    for copy in up_routed(k * experts + g * 2 + u):
                        copy.wait()
                for u in range(2):
                    e = g * 2 + u
                    q = k * experts + e

                    def put(i, cols, d):
                        acc = (acc1, acc3)[i]
                        acc[e, :, cols] = d + jnp.where(k == 0, 0.0, acc[e, :, cols])

                    two_products(
                        abuf, xg[pl.ds(pl.multiple_of(e * CAP, CAP), CAP), :], lax.rem(q, UP_SLOTS), put
                    )
                for u in range(2):
                    start_up(k * experts + g * 2 + u + UP_SLOTS)
                if last:
                    for u in range(2):
                        e = g * 2 + u
                        inner[e] = (jax.nn.silu(acc1[e]) * acc3[e]).astype(BF16)
                    return 0

                @pl.when(g == 1)
                def _():
                    forward_far(k + 1)

                @pl.when((g == 1) & (k + 2 < K_CHUNKS))
                def _():
                    forward_near(k + 2)

                return 0

            with jax.named_scope('up_steps'):
                lax.fori_loop(0, experts // 2, up_step, 0)

        def up_chunk_step(k, _):
            up_chunk(k, False)
            return 0

        lax.fori_loop(0, K_CHUNKS - 1, up_chunk_step, 0)
        up_chunk(jnp.int32(K_CHUNKS - 1), True)
        for i in range(1, n):
            info_copy(i, me, lax.rem(me + i, n)).wait_send()
        for k in range(K_CHUNKS):
            for lane_i in range(7):
                rows_copy(jnp.int32(k), me, lane_i, sib).wait_send()

    def phase_two(ebuf, part, sacc1, sacc3, sinner, sh, obuf, sbuf):
        def shared_product(s, buf, slot):
            k, h = s // halves, lax.rem(s, halves)

            def put(i, cols, d):
                acc = (sacc1, sacc3)[i]
                acc[h, :, cols] = d + jnp.where(k == 0, 0.0, acc[h, :, cols])

            two_products(buf, x_all[k, block(me), :], slot, put)

        def late_copies(i):
            slot = lax.rem(i, LATE_SLOTS)
            return [
                pltpu.make_async_copy(src, sbuf.at[slot, m], s_sem.at[slot, m]) for m, src in enumerate(shared_src(i))
            ]

        def late_turn(t):
            @pl.when(t + 1 < N_CHUNKS)
            def _():
                for i in range(turn):
                    late_start((t + 1) * turn + i)

            with jax.named_scope('late_shared'):
                for i in range(turn):
                    for copy in late_copies(t * turn + i):
                        copy.wait()
                for i in range(turn):
                    shared_product(t * turn + i, sbuf, lax.rem(t * turn + i, LATE_SLOTS))

        def late_start(i):
            for copy in late_copies(i):
                copy.start()

        for i in range(turn):
            late_start(jnp.int32(i))

        def sib_copy(j, c):
            return remote(
                part.at[j, block(c * 2 + (1 - core))], from_sib.at[j, c], sib_send.at[j, c], sib_recv.at[j, c], sib
            )

        def step_of(j):
            return 1 - 2 * lax.rem(j, 2)

        def tr_copy(j):
            d = step_of(j)
            return remote(part.at[j, block(far)], from_tr.at[j], tr_send.at[j], tr_recv.at[j], dev(chip + d, core))

        def dir_copy(j):
            to = dev(chip - step_of(j), core)
            return remote(part.at[j, block(to)], from_fin.at[1, j], dir_send.at[j], fin_recv.at[1, j], to)

        def com_copy(j):
            to = dev(chip + step_of(j), core)
            return remote(part.at[j, block(to)], from_fin.at[0, j], com_send.at[j], fin_recv.at[0, j], to)

        def products(t, half):
            buf = (bbuf, bbuf_hi)[half]
            with jax.named_scope('products'):
                for slot in range(slots):
                    e = half * slots + slot
                    down_routed(t, e, buf, slot, e).wait()
                for slot in range(slots):
                    e = half * slots + slot
                    d = jnp.dot(inner[e], buf[slot], preferred_element_type=F32)
                    ebuf[t, e] = d.astype(BF16)

                @pl.when(t + 1 < N_CHUNKS)
                def _():
                    for slot in range(slots):
                        e = half * slots + slot
                        down_routed(t + 1, e, buf, slot, e).start()

                @pl.when(t + 1 == N_CHUNKS)
                def _():
                    for slot in range(slots):
                        e = half * slots + slot
                        down_shared(e, buf, slot, e).start()

        def spread(t, c):
            span = pl.ds(pl.multiple_of(c * 2 * rows, 32), 2 * rows)
            with jax.named_scope('spread'):
                acc = jnp.zeros((2 * rows, nd), F32)
                for e in range(experts):
                    d = jnp.dot(ssel[e, span, :], ebuf[t, e], preferred_element_type=F32)
                    wt = wb[e, span, :]
                    if nd > 128:
                        wt = jnp.concatenate([wt] * (nd // 128), axis=1)
                    acc = acc + d * wt
                for i in range(per):
                    part[t * per + i, span, :] = acc[:, i * jd : (i + 1) * jd]
            for i in range(per):
                sib_copy(t * per + i, c).start()

        def shared_down(i, half):
            buf = (bbuf, bbuf_hi)[half]
            t = half * (N_CHUNKS // 2) + i
            with jax.named_scope('shared_down'):
                acc = jnp.zeros((rows, nd), F32)
                for h in range(halves):
                    slot = i * halves + h
                    q = half * slots + slot
                    down_shared(q, buf, slot, q).wait()
                    acc = acc + jnp.dot(sinner[h], buf[slot], preferred_element_type=F32)
                for k in range(per):
                    sh[t * per + k] = acc[:, k * jd : (k + 1) * jd]

        def add_sib(t, c):
            with jax.named_scope('add_sib'):
                for i in range(per):
                    j = t * per + i
                    sib_copy(j, c).wait_recv()
                    at = (j, block(c * 2 + core))
                    part[at] = part[at] + from_sib[j, c]

        def near_home(t):
            add_sib(t, chip_right)
            add_sib(t, chip_left)
            for i in range(per):
                dir_copy(t * per + i).start()

        def far_onward(t):
            add_sib(t, chip_far)
            for i in range(per):
                tr_copy(t * per + i).start()

        def far_home(t):
            for i in range(per):
                j = t * per + i
                with jax.named_scope('add_tr'):
                    tr_copy(j).wait_recv()
                    at = (j, block(dev(chip + step_of(j), core)))
                    part[at] = part[at] + from_tr[j]
                com_copy(j).start()

        chip_right, chip_left, chip_far = (lax.rem(chip + i, chips) for i in (1, chips - 1, 2))

        def down_range(t, _):
            products(t, 0)

            @pl.when(t >= 1)
            def _():
                near_home(t - 1)

            products(t, 1)

            spread(t, chip_far)

            def near(i, _):
                spread(t, lax.rem(chip + 1 + 2 * i, chips))
                return 0

            lax.fori_loop(0, 2, near, 0)
            far_onward(t)

            @pl.when(t >= 1)
            def _():
                late_turn(t - 1)

            @pl.when(t >= 1)
            def _():
                far_home(t - 1)

            return 0

        lax.fori_loop(0, N_CHUNKS, down_range, 0)
        last = jnp.int32(N_CHUNKS - 1)
        near_home(last)

        def own_spread(t, _):
            spread(t, chip)
            return 0

        lax.fori_loop(0, N_CHUNKS, own_spread, 0)
        late_turn(last)
        for h in range(halves):
            sinner[h] = (jax.nn.silu(sacc1[h]) * sacc3[h]).astype(BF16)
        for half in range(2):

            def shared_range(i, _):
                shared_down(i, half)
                return 0

            lax.fori_loop(0, N_CHUNKS // 2, shared_range, 0)
            if half == 0:
                far_home(last)

        def own_sums(t, _):
            add_sib(t, chip)
            return 0

        lax.fori_loop(0, N_CHUNKS, own_sums, 0)

        for j in range(J_CHUNKS):
            cols = slice(j * jd, (j + 1) * jd)
            with jax.named_scope('home'):
                com_copy(jnp.int32(j)).wait_recv()
                dir_copy(jnp.int32(j)).wait_recv()
            routed = part[j, block(me), :] + (from_fin[0, j] + from_fin[1, j])
            shared_out = sh[j].astype(BF16).astype(F32)
            obuf[:, cols] = (hid[:, cols].astype(F32) + shared_out + routed).astype(BF16)
            pltpu.make_async_copy(obuf.at[:, cols], out_ref.at[:, cols], out_sem.at[j]).start()

        with jax.named_scope('sent'):
            over_copy.wait()
            for j in range(J_CHUNKS):
                ji = jnp.int32(j)
                for c in range(chips):
                    sib_copy(ji, c).wait_send()
                tr_copy(ji).wait_send()
                dir_copy(ji).wait_send()
                com_copy(ji).wait_send()
            for j in range(J_CHUNKS):
                cols = slice(j * jd, (j + 1) * jd)
                pltpu.make_async_copy(obuf.at[:, cols], out_ref.at[:, cols], out_sem.at[j]).wait()

    pl.run_scoped(
        phase_one,
        pltpu.VMEM((experts * CAP, kd), BF16),
        pltpu.VMEM((experts * CAP, total), BF16),
        pltpu.VMEM((experts, CAP, ff), F32),
        pltpu.VMEM((experts, CAP, ff), F32),
        pltpu.VMEM((UP_SLOTS, 2, kd, ff), BF16),
    )
    pl.run_scoped(
        phase_two,
        pltpu.VMEM((N_CHUNKS, experts, CAP, nd), BF16),
        pltpu.VMEM((J_CHUNKS, total, jd), F32),
        pltpu.VMEM((halves, rows, ff), F32),
        pltpu.VMEM((halves, rows, ff), F32),
        pltpu.VMEM((halves, rows, ff), BF16),
        pltpu.VMEM((J_CHUNKS, rows, jd), F32),
        pltpu.VMEM((rows, width), BF16),
        pltpu.VMEM((LATE_SLOTS, 2, kd, ff), BF16),
    )


def routed_layer(n, *args):
    hidden, norm_gain, w_gate, w1_shared, w3_shared, w2_shared, w1_experts, w3_experts, w2_experts, topk_ids = args
    rows, width = hidden.shape
    experts, _, ff = w1_experts.shape
    total = n * rows
    chips = n // 2
    kd = width // K_CHUNKS
    jd = width // J_CHUNKS
    nd = width // N_CHUNKS
    halves = w1_shared.shape[1] // ff
    dma = pltpu.SemaphoreType.DMA
    vmem = pltpu.VMEM
    scratch = [
        vmem((rows, width), BF16),
        vmem((width // 128, 128), BF16),
        vmem(w_gate.shape[::-1], BF16),
        vmem(topk_ids.shape[::-1], jnp.int32),
        vmem((128, 128), F32),
        vmem((n, 16, 128), F32),
        vmem((total, 128), F32),
        vmem((total, 128), F32),
        vmem((K_CHUNKS, total, kd), BF16),
        vmem((experts, total, CAP), BF16),
        vmem((experts, total, 128), F32),
        vmem((experts, CAP, ff), BF16),
        vmem((J_CHUNKS, chips, rows, jd), F32),
        vmem((J_CHUNKS, rows, jd), F32),
        vmem((2, J_CHUNKS, rows, jd), F32),
        vmem((experts // 2, ff, nd), BF16),
        vmem((experts // 2, ff, nd), BF16),
        pltpu.SMEM((1, 1), jnp.int32),
        dma((4,)),
        dma((n,)),
        dma((n,)),
        dma((K_CHUNKS, 7)),
        dma((K_CHUNKS, n)),
        dma((UP_SLOTS, 2)),
        dma((LATE_SLOTS, 2)),
        dma((experts,)),
        dma((J_CHUNKS, chips)),
        dma((J_CHUNKS, chips)),
        dma((J_CHUNKS,)),
        dma((J_CHUNKS,)),
        dma((J_CHUNKS,)),
        dma((J_CHUNKS,)),
        dma((2, J_CHUNKS)),
        dma((J_CHUNKS,)),
        dma(()),
    ]
    return pl.pallas_call(
        functools.partial(moe_kernel, n),
        out_shape=[jax.ShapeDtypeStruct((rows, width), BF16), jax.ShapeDtypeStruct((1, 1), jnp.int32)],
        in_specs=[pl.BlockSpec(memory_space=pl.ANY)] * 10,
        out_specs=[pl.BlockSpec(memory_space=pl.ANY), pl.BlockSpec(memory_space=pl.ANY)],
        scratch_shapes=scratch,
        compiler_params=pltpu.CompilerParams(collective_id=0, has_side_effects=True, vmem_limit_bytes=67043328),
        name='moe_layer',
    )(hidden, norm_gain.reshape(-1, 128), w_gate.T, *args[3:9], topk_ids.T)


def solution(mesh):
    n = mesh.shape['ep']
    tok_spec = P(('dp', 'ep'), None)
    expert_spec = P('ep', None, None)

    def local_fn(*args):
        out, over = routed_layer(n, *args)
        return lax.switch(over[0, 0], (lambda: out, lambda: dense_path(n, *args)))

    return jax.shard_map(local_fn, mesh=mesh, in_specs=(tok_spec, P(), P(), P(), P(), P(), expert_spec, expert_spec, expert_spec, tok_spec), out_specs=tok_spec, check_vma=False)
```
